32 devices in a mesh: dp: 2 (over x), ep: 16 (over z, y, core).
Axes of the slice: x: 2, y: 2, z: 4, core: 2. Of those that a mesh axis runs over, the one named last changes fastest.
Arguments:
- x0: bfloat16 [2048, 1024], P(('dp', 'ep')), parts along dimension 0
- idx_a: int32 [2048, 8], P(('dp', 'ep')), parts along dimension 0
- g_a: float32 [2048, 8], P(('dp', 'ep')), parts along dimension 0
- idx_b: int32 [2048, 8], P(('dp', 'ep')), parts along dimension 0
- g_b: float32 [2048, 8], P(('dp', 'ep')), parts along dimension 0
- dy: bfloat16 [2048, 1024], P(('dp', 'ep')), parts along dimension 0
- w1_a: bfloat16 [32, 1024, 512], P('ep')
- w3_a: bfloat16 [32, 1024, 512], P('ep')
- w2_a: bfloat16 [32, 512, 1024], P('ep')
- w1_b: bfloat16 [32, 1024, 512], P('ep')
- w3_b: bfloat16 [32, 1024, 512], P('ep')
- w2_b: bfloat16 [32, 512, 1024], P('ep')
Outputs:
- output 1: bfloat16 [2048, 1024], P(('dp', 'ep')), parts along dimension 0
- output 2: bfloat16 [2048, 1024], P(('dp', 'ep')), parts along dimension 0
- output 3: float32 [64, 1024, 512], P(('dp', 'ep')), parts along dimension 0
- output 4: float32 [64, 1024, 512], P(('dp', 'ep')), parts along dimension 0
- output 5: float32 [64, 512, 1024], P(('dp', 'ep')), parts along dimension 0
- output 6: float32 [64, 1024, 512], P(('dp', 'ep')), parts along dimension 0
- output 7: float32 [64, 1024, 512], P(('dp', 'ep')), parts along dimension 0
- output 8: float32 [64, 512, 1024], P(('dp', 'ep')), parts along dimension 0
- output 9: float32 [2048, 8], P(('dp', 'ep')), parts along dimension 0
- output 10: float32 [2048, 8], P(('dp', 'ep')), parts along dimension 0
There are 2 independent parts. The reference program is written for one: setup_inputs(seed, part) draws one part's arguments, and reference() takes and returns one part's arrays. A program takes and returns all parts, laid end to end along the dimension named above; an argument that names none is the same for every part.
All inputs are finite; a program needn't handle non-finite values.
Results may differ from the reference program's by a relative error of at most 0.00872247.
Values are sent between devices in bfloat16 or wider.
A program may use at most 1 GiB of HBM per device.

```python
import jax
import jax.numpy as jnp
from jax import lax

T = 64
EP = 16
D = 1024
F = 512
E = 32
K = 8
C = 32

N = EP * T


def _levels(key):
    return jnp.sum(jax.random.randint(key, (3, E), 0, 5), axis=0).astype(jnp.uint32)


def _route(key, levels):
    weight = jnp.left_shift(jnp.uint32(1), levels)

    def advance(counts, sub_key):
        wait_time = (jax.random.bits(sub_key, (E,), jnp.uint32) >> 14) * weight
        wait_time = jnp.where(counts < C, wait_time, jnp.uint32(0xFFFFFFFF))
        chosen = jnp.argsort(wait_time)[:K].astype(jnp.int32)
        return counts.at[chosen].add(1), chosen
    return lax.scan(advance, jnp.zeros((E,), jnp.int32), jax.random.split(key, T))[1].astype(jnp.int32)


def _weights(key):
    k1, k3, k2 = jax.random.split(key, 3)
    w1 = (jax.random.normal(k1, (E, D, F), jnp.float32) * D ** -0.5).astype(jnp.bfloat16)
    w3 = (jax.random.normal(k3, (E, D, F), jnp.float32) * D ** -0.5).astype(jnp.bfloat16)
    w2 = (jax.random.normal(k2, (E, F, D), jnp.float32) * F ** -0.5).astype(jnp.bfloat16)
    return w1, w3, w2


def setup_inputs(seed: int = 0, part: int = 0) -> dict:
    key = jax.random.PRNGKey(seed)
    kw_a, kw_b, kp = jax.random.split(key, 3)
    kp = jax.random.fold_in(kp, part)
    kx, kdy, kga, kgb, _, _ = jax.random.split(kp, 6)
    kra, krb, kpa, kpb = jax.random.split(jax.random.fold_in(kp, 7), 4)
    pop_a = _levels(kpa)
    pop_b = _levels(kpb)
    w1_a, w3_a, w2_a = _weights(kw_a)
    w1_b, w3_b, w2_b = _weights(kw_b)
    return {
        'x0': jax.random.normal(kx, (N, D), jnp.float32).astype(jnp.bfloat16),
        'idx_a': jax.vmap(lambda sub_key: _route(sub_key, pop_a))(jax.random.split(kra, EP)).reshape(N, K),
        'g_a': jax.random.uniform(kga, (N, K), jnp.float32, 0.5, 1.0),
        'idx_b': jax.vmap(lambda sub_key: _route(sub_key, pop_b))(jax.random.split(krb, EP)).reshape(N, K),
        'g_b': jax.random.uniform(kgb, (N, K), jnp.float32, 0.5, 1.0),
        'dy': jax.random.normal(kdy, (N, D), jnp.float32).astype(jnp.bfloat16),
        'w1_a': w1_a, 'w3_a': w3_a, 'w2_a': w2_a,
        'w1_b': w1_b, 'w3_b': w3_b, 'w2_b': w2_b,
    }


def _slots(e):
    oh = (e[..., None] == jnp.arange(E)).astype(jnp.int32)
    return jnp.sum(jnp.cumsum(oh, axis=1) * oh, axis=2) - 1


def _pairs(x):
    return jnp.repeat(x.reshape((EP, T) + x.shape[1:]), K, axis=1)


def _dispatch(rows, e, s):
    src = jnp.arange(EP)[:, None]
    buf = jnp.zeros((E, EP, C) + rows.shape[2:], rows.dtype).at[e, src, s].set(rows)
    return buf.reshape((E, EP * C) + rows.shape[2:])


def _collect(buf, e, s):
    buf = buf.reshape((E, EP, C) + buf.shape[2:])
    return buf[e, jnp.arange(EP)[:, None], s]


def _hidden(u, w1, w3):
    a1 = jnp.dot(u, w1, preferred_element_type=jnp.float32)
    a3 = jnp.dot(u, w3, preferred_element_type=jnp.float32)
    sg = jax.nn.sigmoid(a1)
    sl = a1 * sg
    return a1, a3, sg, sl, (sl * a3).astype(jnp.bfloat16)


def _fwd(x, e, s, g, w1, w3, w2):
    u = _dispatch(_pairs(x), e, s)

    def one(a):
        ui, w1i, w3i, w2i = a
        h = _hidden(ui, w1i, w3i)[4]
        return jnp.dot(h, w2i, preferred_element_type=jnp.float32).astype(jnp.bfloat16)
    o = _collect(lax.map(one, (u, w1, w3, w2)), e, s).reshape(N, K, D)
    y = x.astype(jnp.float32) + jnp.sum(g[:, :, None] * o.astype(jnp.float32), axis=1)
    return y.astype(jnp.bfloat16)


def _bwd(x, z, e, s, g, w1, w3, w2):
    u = _dispatch(_pairs(x), e, s)
    zb = _dispatch(_pairs(z), e, s)
    gb = _dispatch(g.reshape(EP, T * K), e, s)

    def one(a):
        ui, zi, gi, w1i, w3i, w2i = a
        a1, a3, sg, sl, h = _hidden(ui, w1i, w3i)
        r = jnp.dot(zi, w2i.T, preferred_element_type=jnp.float32)
        dg = jnp.sum(h.astype(jnp.float32) * r, axis=1)
        gi = gi[:, None]
        do = (gi * zi.astype(jnp.float32)).astype(jnp.bfloat16)
        dw2 = jnp.dot(h.T, do, preferred_element_type=jnp.float32)
        dh = gi * r
        da3 = (dh * sl).astype(jnp.bfloat16)
        da1 = (dh * a3 * sg * (1.0 + a1 * (1.0 - sg))).astype(jnp.bfloat16)
        dw1 = jnp.dot(ui.T, da1, preferred_element_type=jnp.float32)
        dw3 = jnp.dot(ui.T, da3, preferred_element_type=jnp.float32)
        du = (jnp.dot(da1, w1i.T, preferred_element_type=jnp.float32)
              + jnp.dot(da3, w3i.T, preferred_element_type=jnp.float32)).astype(jnp.bfloat16)
        return dw1, dw3, dw2, du, dg
    dw1, dw3, dw2, du, dg = lax.map(one, (u, zb, gb, w1, w3, w2))
    du = _collect(du, e, s).reshape(N, K, D)
    dx = (z.astype(jnp.float32) + jnp.sum(du.astype(jnp.float32), axis=1)).astype(jnp.bfloat16)
    return dx, dw1, dw3, dw2, _collect(dg, e, s).reshape(N, K)


def reference(x0, idx_a, g_a, idx_b, g_b, dy, w1_a, w3_a, w2_a, w1_b, w3_b, w2_b):
    ea = idx_a.reshape(EP, T * K)
    eb = idx_b.reshape(EP, T * K)
    sa = _slots(ea)
    sb = _slots(eb)
    x1 = _fwd(x0, ea, sa, g_a, w1_a, w3_a, w2_a)
    x2 = _fwd(x1, eb, sb, g_b, w1_b, w3_b, w2_b)
    dx1, dw1_b, dw3_b, dw2_b, dg_b = _bwd(x1, dy, eb, sb, g_b, w1_b, w3_b, w2_b)
    dx0, dw1_a, dw3_a, dw2_a, dg_a = _bwd(x0, dx1, ea, sa, g_a, w1_a, w3_a, w2_a)
    return (x2, dx0, dw1_a, dw3_a, dw2_a, dw1_b, dw3_b, dw2_b, dg_a, dg_b)
```

```python
import jax
import jax.numpy as jnp
from jax import lax
from jax.sharding import PartitionSpec as P

F32 = jnp.float32
BF = jnp.bfloat16


def _gates(idx, g, n_exp, el):
    m = idx[:, :, None] == jnp.arange(n_exp)
    gm = jnp.max(jnp.where(m, g[:, :, None], -1.0), axis=1)
    gm = lax.all_gather(gm, 'ep', axis=0, tiled=True)
    i = lax.axis_index('ep')
    return lax.dynamic_slice_in_dim(gm, i * el, el, axis=1).T


def _hidden(u, w1, w3):
    a1 = jnp.einsum('rd,edf->erf', u, w1, preferred_element_type=F32)
    a3 = jnp.einsum('rd,edf->erf', u, w3, preferred_element_type=F32)
    sg = jax.nn.sigmoid(a1)
    sl = a1 * sg
    return a1, a3, sg, sl, (sl * a3).astype(BF)


def _forward(x, u, gc, w1, w3, w2):
    gc = gc[:, :, None]
    h = _hidden(u, w1, w3)[4]
    o = jnp.einsum('erf,efd->erd', h, w2, preferred_element_type=F32).astype(BF)
    y = jnp.sum(jnp.where(gc >= 0, gc * o.astype(F32), 0.0), axis=0)
    y = lax.psum_scatter(y, 'ep', scatter_dimension=0, tiled=True)
    return (x.astype(F32) + y).astype(BF)


def _backward(u, z, zb, idx, gc, w1, w3, w2):
    el = w1.shape[0]
    gc = gc[:, :, None]
    ok = gc >= 0
    a1, a3, sg, sl, h = _hidden(u, w1, w3)
    h = jnp.where(ok, h, jnp.zeros_like(h))
    r = jnp.einsum('rd,efd->erf', zb, w2, preferred_element_type=F32)
    dg = jnp.sum(jnp.where(ok, h.astype(F32) * r, 0.0), axis=2)
    do = jnp.where(ok, gc * zb.astype(F32)[None], 0.0).astype(BF)
    dw2 = jnp.einsum('erf,erd->efd', h, do, preferred_element_type=F32)
    dh = gc * r
    da3 = jnp.where(ok, dh * sl, 0.0).astype(BF)
    da1 = jnp.where(ok, dh * a3 * sg * (1.0 + a1 * (1.0 - sg)), 0.0).astype(BF)
    dw1 = jnp.einsum('rd,erf->edf', u, da1, preferred_element_type=F32)
    dw3 = jnp.einsum('rd,erf->edf', u, da3, preferred_element_type=F32)
    du = (jnp.einsum('erf,edf->erd', da1, w1, preferred_element_type=F32)
          + jnp.einsum('erf,edf->erd', da3, w3, preferred_element_type=F32)).astype(BF)
    du = lax.psum_scatter(jnp.sum(du.astype(F32), axis=0), 'ep', scatter_dimension=0, tiled=True)
    dx = (z.astype(F32) + du).astype(BF)
    t = z.shape[0]
    dg = lax.all_to_all(dg.reshape(el, -1, t), 'ep', 1, 0, tiled=True)
    dg = dg.reshape(-1, t)
    dgt = jnp.sum(jnp.where(idx[:, :, None] == jnp.arange(dg.shape[0]), dg.T[:, None, :], 0.0), axis=2)
    return dx, dw1, dw3, dw2, dgt


def solution(mesh):
    tok = P(('dp', 'ep'))
    wsp = P('ep')
    c = mesh.shape['ep']

    def body(x0, idx_a, g_a, idx_b, g_b, dy, w1_a, w3_a, w2_a, w1_b, w3_b, w2_b):
        el = w1_a.shape[0]
        ga = _gates(idx_a, g_a, el * c, el)
        gb = _gates(idx_b, g_b, el * c, el)
        ag = lambda v: lax.all_gather(v, 'ep', axis=0, tiled=True)
        u0 = ag(x0)
        zb = ag(dy)
        x1 = _forward(x0, u0, ga, w1_a, w3_a, w2_a)
        u1 = ag(x1)
        x2 = _forward(x1, u1, gb, w1_b, w3_b, w2_b)
        dx1, dw1_b, dw3_b, dw2_b, dg_b = _backward(u1, dy, zb, idx_b, gb, w1_b, w3_b, w2_b)
        dx0, dw1_a, dw3_a, dw2_a, dg_a = _backward(u0, dx1, ag(dx1), idx_a, ga, w1_a, w3_a, w2_a)
        return x2, dx0, dw1_a, dw3_a, dw2_a, dw1_b, dw3_b, dw2_b, dg_a, dg_b

    return jax.shard_map(body, mesh=mesh,
                         in_specs=(tok,) * 6 + (wsp,) * 6,
                         out_specs=(tok,) * 10,
                         check_vma=False)
```

```python
import jax
import jax.numpy as jnp
from jax import lax
from jax.experimental import pallas as pl
from jax.experimental.pallas import tpu as pltpu
from jax.sharding import PartitionSpec as P

F32 = jnp.float32
BF = jnp.bfloat16
MESH = pl.DeviceIdType.MESH
VMEM_LIMIT = 67043328

REL = (4, 3, -3, 2, -2, 1, -1, 0)
UP = (0, 1, 3, 5, 7)
DOWN = (0, 2, 4, 6, 7)


def _ring_pos(ep):
    z, y = ep // 4, (ep // 2) % 2
    return z + y * (7 - 2 * z)


def _ring_ep(pos, core):
    y = pos // 4
    z = pos + y * (7 - 2 * pos)
    return z * 4 + y * 2 + core


def _nt(a, b):
    return lax.dot_general(a, b, (((1,), (1,)), ((), ())), preferred_element_type=F32)


def _nn(a, b):
    return jnp.dot(a, b, preferred_element_type=F32)


def _main_kernel(x0_ref, dy_ref, gt_ref, w1a_h, w3a_h, w2a_h, w1b_h, w3b_h, w2b_h,
                 x2_ref, dx0_ref, dgr_ref, gc_ref, xg_o, zg_o, h_o, da1_o, da3_o,
                 w1, w3, w2, xg, ps, dr, ru, rd, a1s, a3s, hs, d1s, d3s, gtr, dgc, dgs,
                 wsem, ag_s, ag_r, ax_s, ax_r, rs_s, rs_r, rx_s, rx_r, g_s, g_r, d_s, d_r, osem):
    T = x0_ref.shape[0]
    H = T // 2
    me = lax.axis_index('ep')
    core = me % 2
    pos = _ring_pos(me)
    up = _ring_ep((pos + 1) % 8, core)
    down = _ring_ep((pos + 7) % 8, core)
    mate = me + 1 - 2 * core

    wcopies = []
    for l, refs in enumerate(((w1a_h, w3a_h, w2a_h), (w1b_h, w3b_h, w2b_h))):
        for i, (src, dst) in enumerate(zip(refs, (w1, w3, w2))):
            c = pltpu.make_async_copy(src, dst.at[l], wsem.at[l * 3 + i])
            c.start()
            wcopies.append(c)

    bar = pltpu.get_barrier_semaphore()
    for i in range(1, 16):
        pl.semaphore_signal(bar, inc=1, device_id={'ep': (me + i) % 16}, device_id_type=MESH)
    pl.semaphore_wait(bar, 15)

    def rcopy(src, dst, ss, rs, dev):
        return pltpu.make_async_remote_copy(src_ref=src, dst_ref=dst, send_sem=ss, recv_sem=rs,
                                            device_id={'ep': dev}, device_id_type=MESH)

    def half(i):
        return pl.ds(i * H, H)

    pending = []

    def ag_msgs(n):
        buf = xg.at[n]
        u, d, m = [], [], []
        usl, dsl = (7, 6, 4, 2, 0), (7, 5, 3, 1, 0)
        for j in range(7):
            hu, hd = j % 2, 1 - j % 2
            u.append(rcopy(buf.at[usl[j // 2], 0, half(hu)], buf.at[usl[j // 2 + 1], 0, half(hu)],
                           ag_s.at[n, 0, j], ag_r.at[n, 0, j], up))
            d.append(rcopy(buf.at[dsl[j // 2], 0, half(hd)], buf.at[dsl[j // 2 + 1], 0, half(hd)],
                           ag_s.at[n, 1, j], ag_r.at[n, 1, j], down))
        for k in range(8):
            for hf in range(2):
                m.append(rcopy(buf.at[k, 0, half(hf)], buf.at[k, 1, half(hf)],
                               ax_s.at[n, k * 2 + hf], ax_r.at[n, k * 2 + hf], mate))
        return u, d, m

    def ag_start(n):
        u, d, m = ag_msgs(n)
        for j in range(2):
            u[j].start()
            d[j].start()
        for hf in range(2):
            m[7 * 2 + hf].start()
        return u, d, m

    def ag_finish(msgs):
        u, d, m = msgs
        usl, dsl = (6, 4, 2, 0), (5, 3, 1, 0)
        for j in range(7):
            u[j].wait_recv()
            if j + 2 < 7:
                u[j + 2].start()
            m[usl[j // 2] * 2 + j % 2].start()
            d[j].wait_recv()
            if j + 2 < 7:
                d[j + 2].start()
            m[dsl[j // 2] * 2 + 1 - j % 2].start()
        for c in m:
            c.wait_recv()
        pending.extend(u + d + m)

    def rs_local_msgs(n, b):
        return [rcopy(ps.at[b, pl.ds(2 * ch, 2), 1], dr.at[b, pl.ds(2 * ch, 2)],
                      rx_s.at[n, ch], rx_r.at[n, ch], mate) for ch in range(4)]

    def rs_msgs(n, b):
        u, d = [], []
        for j in range(7):
            k = (j + 1) // 2
            hu, hd = j % 2, 1 - j % 2
            u.append(rcopy(ps.at[b, UP[k], 0, half(hu)], ru.at[b, j], rs_s.at[n, 0, j], rs_r.at[n, 0, j], up))
            d.append(rcopy(ps.at[b, DOWN[k], 0, half(hd)], rd.at[b, j], rs_s.at[n, 1, j], rs_r.at[n, 1, j], down))
        return u, d

    def rs_run(n, b, loc):
        u, d = rs_msgs(n, b)

        def merge(ch):
            loc[ch].wait_recv()
            for k in (2 * ch, 2 * ch + 1):
                ps[b, k, 0] += dr[b, k]
        merge(0)
        u[0].start()
        d[0].start()
        u[1].start()
        merge(1)
        d[1].start()
        merge(2)
        merge(3)
        for j in range(7):
            k = (j + 3) // 2
            hu, hd = j % 2, 1 - j % 2
            u[j].wait_recv()
            ps[b, UP[k], 0, half(hu)] += ru[b, j]
            if j + 2 < 7:
                u[j + 2].start()
            d[j].wait_recv()
            ps[b, DOWN[k], 0, half(hd)] += rd[b, j]
            if j + 2 < 7:
                d[j + 2].start()
        pending.extend(u + d + loc)

    def drain():
        for c in pending:
            c.wait_send()
        pending.clear()

    xg[0, 7, 0] = x0_ref[...]
    xg[1, 7, 0] = dy_ref[...]
    msgs0 = ag_start(0)
    gmsgs = []
    for k in range(8):
        q = (pos - REL[k] + 8) % 8
        for plane in range(2):
            if k == 7 and plane == 0:
                continue
            dev = _ring_ep(q, core + plane * (1 - 2 * core))
            c = rcopy(gt_ref.at[pl.ds(dev * 8, 8)], gtr.at[pl.ds((k * 2 + plane) * 8, 8)],
                      g_s.at[k * 2 + plane], g_r.at[k * 2 + plane], dev)
            c.start()
            gmsgs.append(c)
    gtr[14 * 8:15 * 8] = gt_ref[pl.ds(pl.multiple_of(me * 8, 8), 8)]
    ag_finish(msgs0)
    msgs1 = ag_start(1)
    for c in gmsgs:
        c.wait_recv()
    pending.extend(gmsgs)
    gct = gtr[...].T
    for b in range(16):
        gc_ref[b * T:(b + 1) * T, 0:8] = gct[0:T, b * 8:b * 8 + 8]

    R = 4 * T

    def hidden(n, l, e, rows, mask):
        u = rows_of(n, rows)
        a1 = _nn(u, w1[l, e])
        a3 = _nn(u, w3[l, e])
        sg = 1.0 / (1.0 + jnp.exp(-a1))
        sl = a1 * sg
        h = jnp.where(mask, sl * a3, 0.0).astype(BF)
        return a1, a3, sg, sl, h

    def rows_of(n, ch):
        return xg[n, pl.ds(2 * ch, 2)].reshape(R, -1)

    def put(b, ch, e, v):
        v = v.reshape(2, 2, T, v.shape[-1])
        if e == 0:
            ps[b, pl.ds(2 * ch, 2)] = v
        else:
            ps[b, pl.ds(2 * ch, 2)] += v

    def rowslice(ch):
        return pl.ds(pl.multiple_of(ch * R, R), R)

    for c in wcopies[:3]:
        c.wait()
    loc = rs_local_msgs(0, 0)

    @pl.loop(0, 4)
    def _(ch):
        rows = rowslice(ch)
        for e in range(2):
            g = gc_ref[rows, e:e + 1]
            a1, a3, sg, sl, h = hidden(0, 0, e, ch, g >= 0)
            a1s[e, rows] = a1
            a3s[e, rows] = a3
            o = _nn(h, w2[0, e]).astype(BF).astype(F32)
            put(0, ch, e, g * o)
    for c in loc:
        c.start()
    ag_finish(msgs1)
    rs_run(0, 0, loc)
    xg[2, 7, 0] = (x0_ref[...].astype(F32) + ps[0, 7, 0]).astype(BF)
    ag_finish(ag_start(2))
    drain()

    def back(l, nz, b, ch, rows, e, g, a1, a3, sg, sl, h):
        mask = g >= 0
        r = _nt(rows_of(nz, ch), w2[l, e])
        dgc[rows, 2 * l + e:2 * l + e + 1] = jnp.sum(h.astype(F32) * r, axis=1, keepdims=True)
        dh = g * r
        da3 = jnp.where(mask, dh * sl, 0.0).astype(BF)
        da1 = jnp.where(mask, dh * a3 * sg * (1.0 + a1 * (1.0 - sg)), 0.0).astype(BF)
        hs[l, e, rows] = h
        d1s[l, e, rows] = da1
        d3s[l, e, rows] = da3
        du = (_nt(da1, w1[l, e]) + _nt(da3, w3[l, e])).astype(BF).astype(F32)
        put(b, ch, e, du)

    for c in wcopies[3:]:
        c.wait()
    locx = rs_local_msgs(1, 1)
    loc = rs_local_msgs(2, 0)

    @pl.loop(0, 4)
    def _(ch):
        rows = rowslice(ch)
        for e in range(2):
            g = gc_ref[rows, 2 + e:3 + e]
            a1, a3, sg, sl, h = hidden(2, 1, e, ch, g >= 0)
            o = _nn(h, w2[1, e]).astype(BF).astype(F32)
            put(1, ch, e, g * o)
            back(1, 1, 0, ch, rows, e, g, a1, a3, sg, sl, h)
    for c in loc + locx:
        c.start()
    outs = []

    def out(src, dst, i):
        c = pltpu.make_async_copy(src, dst, osem.at[i])
        c.start()
        outs.append(c)
    for i, (s, d) in enumerate(((hs, h_o), (d1s, da1_o), (d3s, da3_o))):
        out(s.at[1], d.at[1], i)
    out(xg.at[0], xg_o.at[0], 3)
    out(xg.at[2], xg_o.at[1], 4)
    out(xg.at[1], zg_o.at[1], 5)
    rs_run(2, 0, loc)
    xg[3, 7, 0] = (dy_ref[...].astype(F32) + ps[0, 7, 0]).astype(BF)
    m3 = ag_start(3)
    ag_finish(m3)
    drain()
    out(xg.at[3], zg_o.at[0], 6)

    loc = rs_local_msgs(3, 0)

    @pl.loop(0, 4)
    def _(ch):
        rows = rowslice(ch)
        for e in range(2):
            g = gc_ref[rows, e:e + 1]
            a1 = a1s[e, rows]
            a3 = a3s[e, rows]
            sg = 1.0 / (1.0 + jnp.exp(-a1))
            sl = a1 * sg
            h = jnp.where(g >= 0, sl * a3, 0.0).astype(BF)
            back(0, 3, 0, ch, rows, e, g, a1, a3, sg, sl, h)
    for c in loc:
        c.start()
    for i, (s, d) in enumerate(((hs, h_o), (d1s, da1_o), (d3s, da3_o))):
        out(s.at[0], d.at[0], 7 + i)

    dmsgs = []
    for k in range(8):
        t = dgc[k * 2 * T:(k + 1) * 2 * T].T[0:8]
        dgs[k * 16:k * 16 + 8] = t
        dgs[k * 16 + 8:k * 16 + 16] = pltpu.roll(t, T, 1)
        q = (pos + REL[k] + 8) % 8
        for plane in range(2):
            b = k * 2 + plane
            if k == 7 and plane == 0:
                continue
            dev = _ring_ep(q, core + plane * (1 - 2 * core))
            c = rcopy(dgs.at[pl.ds(b * 8, 8)], dgr_ref.at[pl.ds(me * 8, 8)], d_s.at[b], d_r.at[b], dev)
            c.start()
            dmsgs.append(c)
    dgr_ref[pl.ds(pl.multiple_of(me * 8, 8), 8)] = dgs[14 * 8:15 * 8]

    rs_run(1, 1, locx)
    x2_ref[...] = (xg[2, 7, 0].astype(F32) + ps[1, 7, 0]).astype(BF)
    rs_run(3, 0, loc)
    dx0_ref[...] = (xg[3, 7, 0].astype(F32) + ps[0, 7, 0]).astype(BF)
    for c in dmsgs:
        c.wait_recv()
    pending.extend(dmsgs)
    drain()
    for c in outs:
        c.wait()


def _main(x0, dy, gt, ws):
    T, D = x0.shape
    EL, _, F = ws[0].shape
    N = 16 * T
    S = jax.ShapeDtypeStruct
    vm = pl.BlockSpec(memory_space=pltpu.VMEM)
    hb = pl.BlockSpec(memory_space=pl.ANY)
    dma = pltpu.SemaphoreType.DMA
    return pl.pallas_call(
        _main_kernel,
        out_shape=(S((T, D), BF), S((T, D), BF), S((128, 128), F32), S((N, 128), F32),
                   S((2, 8, 2, T, D), BF), S((2, 8, 2, T, D), BF),
                   S((2, EL, N, F), BF), S((2, EL, N, F), BF), S((2, EL, N, F), BF)),
        in_specs=[vm] * 3 + [hb] * 6,
        out_specs=(vm, vm, vm, vm) + (hb,) * 5,
        scratch_shapes=[
            pltpu.VMEM((2, EL, D, F), BF), pltpu.VMEM((2, EL, D, F), BF), pltpu.VMEM((2, EL, F, D), BF),
            pltpu.VMEM((4, 8, 2, T, D), BF),
            pltpu.VMEM((2, 8, 2, T, D), F32), pltpu.VMEM((2, 8, T, D), F32),
            pltpu.VMEM((2, 7, T // 2, D), F32), pltpu.VMEM((2, 7, T // 2, D), F32),
            pltpu.VMEM((EL, N, F), F32), pltpu.VMEM((EL, N, F), F32),
            pltpu.VMEM((2, EL, N, F), BF), pltpu.VMEM((2, EL, N, F), BF), pltpu.VMEM((2, EL, N, F), BF),
            pltpu.VMEM((128, 128), F32), pltpu.VMEM((N, 128), F32), pltpu.VMEM((128, 128), F32),
            dma((6,)), dma((4, 2, 7)), dma((4, 2, 7)), dma((4, 16)), dma((4, 16)),
            dma((4, 2, 7)), dma((4, 2, 7)), dma((4, 4)), dma((4, 4)),
            dma((16,)), dma((16,)), dma((16,)), dma((16,)), dma((10,)),
        ],
        compiler_params=pltpu.CompilerParams(collective_id=0, has_side_effects=True,
                                             vmem_limit_bytes=VMEM_LIMIT),
        name='moe',
    )(x0, dy, gt, *ws)


def _tn(a, b):
    return lax.dot_general(a, b, (((0,), (0,)), ((), ())), preferred_element_type=F32)


def _wgrad_kernel(l, xg, zg, gc, h, d1, d3, o1, o3, o2):
    e = pl.program_id(0)
    x = xg[0]
    o1[0] = _tn(x, d1[0, 0])
    o3[0] = _tn(x, d3[0, 0])
    g = jnp.where(e == 0, gc[:, 2 * l:2 * l + 1], gc[:, 2 * l + 1:2 * l + 2])
    do = jnp.where(g >= 0, g * zg[0].astype(F32), 0.0).astype(BF)
    o2[0] = _tn(h[0, 0], do)


def _wgrad(l, xg, zg, gc, h, d1, d3):
    import functools
    _, N, D = xg.shape
    EL, F = h.shape[1], h.shape[3]
    S = jax.ShapeDtypeStruct
    tok = pl.BlockSpec((1, N, D), lambda e: (l, 0, 0))
    act = pl.BlockSpec((1, 1, N, F), lambda e: (l, e, 0, 0))
    return pl.pallas_call(
        functools.partial(_wgrad_kernel, l),
        grid=(EL,),
        out_shape=(S((EL, D, F), F32), S((EL, D, F), F32), S((EL, F, D), F32)),
        in_specs=[tok, tok, pl.BlockSpec((N, 128), lambda e: (0, 0)), act, act, act],
        out_specs=(pl.BlockSpec((1, D, F), lambda e: (e, 0, 0)),) * 2 + (pl.BlockSpec((1, F, D), lambda e: (e, 0, 0)),),
        compiler_params=pltpu.CompilerParams(vmem_limit_bytes=VMEM_LIMIT),
        name='wgrad',
    )(xg, zg, gc, h, d1, d3)


def solution(mesh):
    tok = P(('dp', 'ep'))
    wsp = P('ep')

    def gates(idx, g, ne):
        m = idx[:, :, None] == jnp.arange(ne)
        return jnp.max(jnp.where(m, g[:, :, None], -1.0), axis=1)

    def body(x0, idx_a, g_a, idx_b, g_b, dy, *ws):
        T, D = x0.shape
        EL = ws[0].shape[0]
        ne = 16 * EL
        ga = gates(idx_a, g_a, ne).T.reshape(16, EL, T)
        gb = gates(idx_b, g_b, ne).T.reshape(16, EL, T)
        gt = jnp.concatenate([ga, gb], axis=1)
        gt = jnp.pad(gt, ((0, 0), (0, 8 - 2 * EL), (0, 128 - T)), constant_values=-1.0).reshape(128, 128)
        x2, dx0, dgr, gc, xg, zg, h, d1, d3 = _main(x0, dy, gt, ws)
        N = 16 * T
        xg = xg.reshape(2, N, D)
        zg = zg.reshape(2, N, D)
        dwb = _wgrad(1, xg, zg, gc, h, d1, d3)
        dwa = _wgrad(0, xg, zg, gc, h, d1, d3)

        dgr = dgr.reshape(16, 8, 128)[:, :, :T]

        def dgate(l, idx):
            d = dgr[:, l * EL:(l + 1) * EL].reshape(ne, T).T
            return jnp.sum(jnp.where(idx[:, :, None] == jnp.arange(ne), d[:, None, :], 0.0), axis=2)
        return (x2, dx0) + tuple(dwa) + tuple(dwb) + (dgate(0, idx_a), dgate(1, idx_b))

    return jax.shard_map(body, mesh=mesh,
                         in_specs=(tok,) * 6 + (wsp,) * 6,
                         out_specs=(tok,) * 10,
                         check_vma=False)
```

```python
import jax
import jax.numpy as jnp
from jax import lax
from jax.experimental import pallas as pl
from jax.experimental.pallas import tpu as pltpu
from jax.sharding import PartitionSpec as P

F32 = jnp.float32
BF = jnp.bfloat16
MESH = pl.DeviceIdType.MESH
VMEM_LIMIT = 67043328

REL = (-1, 0, -2, 1, 4, 3, -3, 2)
OWN = 1
UP = (4, 5, 7, 3, 1)
DOWN = (4, 6, 2, 0, 1)


def _ring_pos(ep):
    z, y = ep // 4, (ep // 2) % 2
    return z + y * (7 - 2 * z)


def _ring_ep(pos, core):
    y = pos // 4
    z = pos + y * (7 - 2 * pos)
    return z * 4 + y * 2 + core


def _nt(a, b):
    return lax.dot_general(a, b, (((1,), (1,)), ((), ())), preferred_element_type=F32)


def _nn(a, b):
    return jnp.dot(a, b, preferred_element_type=F32)


def _main_kernel(x0_ref, dy_ref, meta_ref, w1a_h, w3a_h, w2a_h, w1b_h, w3b_h, w2b_h,
                 x2_ref, dx0_ref, dgr_ref, gc_ref, xg_o, zg_o, h_o, da1_o, da3_o,
                 w1, w3, w2, xg, ps, dr, ru, rd, a1s, a3s, hs, d1s, d3s, gts, gtr, dgc, dgs, tmp1, tmp3,
                 wsem, ag_s, ag_r, ax_s, ax_r, rs_s, rs_r, rx_s, rx_r, g_s, g_r, d_s, d_r, osem):
    T = x0_ref.shape[0]
    H = T // 2
    R = 4 * T
    me = lax.axis_index('ep')
    core = me % 2
    pos = _ring_pos(me)
    up = _ring_ep((pos + 1) % 8, core)
    down = _ring_ep((pos + 7) % 8, core)
    mate = me + 1 - 2 * core

    wcopies = []
    for l, refs in enumerate(((w1a_h, w3a_h, w2a_h), (w1b_h, w3b_h, w2b_h))):
        for i, (src, dst) in enumerate(zip(refs, (w1, w3, w2))):
            c = pltpu.make_async_copy(src, dst.at[l], wsem.at[l * 3 + i])
            c.start()
            wcopies.append(c)

    bar = pltpu.get_barrier_semaphore()
    for i in range(1, 16):
        pl.semaphore_signal(bar, inc=1, device_id={'ep': (me + i) % 16}, device_id_type=MESH)
    xg[0, OWN, 0] = x0_ref[...]
    xg[1, OWN, 0] = dy_ref[...]
    for l in range(2):
        idx = meta_ref[8 * l:8 * l + 8]
        gate = meta_ref[16 + 8 * l:24 + 8 * l]
        for i in range(16):
            for e in range(2):
                row = jnp.max(jnp.where(idx == float(2 * i + e), gate, -1.0), axis=0, keepdims=True)
                gts[8 * i + 2 * l + e:8 * i + 2 * l + e + 1] = row
    for i in range(16):
        gts[8 * i + 4:8 * i + 8] = jnp.full((4, 128), -1.0, F32)
    dgc[...] = jnp.zeros_like(dgc)
    pl.semaphore_wait(bar, 15)

    def rcopy(src, dst, ss, rs, dev):
        return pltpu.make_async_remote_copy(src_ref=src, dst_ref=dst, send_sem=ss, recv_sem=rs,
                                            device_id={'ep': dev}, device_id_type=MESH)

    def half(i):
        return pl.ds(i * H, H)

    pending = []

    AU, AD = (1, 0, 2, 6, 4), (1, 3, 7, 5, 4)

    def ag_u(n, j):
        i, h = j // 2, half(j % 2)
        return rcopy(xg.at[n, AU[i], 0, h], xg.at[n, AU[i + 1], 0, h], ag_s.at[n, 0, j], ag_r.at[n, 0, j], up)

    def ag_d(n, j):
        i, h = j // 2, half(1 - j % 2)
        return rcopy(xg.at[n, AD[i], 0, h], xg.at[n, AD[i + 1], 0, h], ag_s.at[n, 1, j], ag_r.at[n, 1, j], down)

    def ag_m(n, k, hf):
        return rcopy(xg.at[n, k, 0, half(hf)], xg.at[n, k, 1, half(hf)],
                     ax_s.at[n, k * 2 + hf], ax_r.at[n, k * 2 + hf], mate)

    def ag_start(n):
        for j in range(2):
            ag_u(n, j).start()
            ag_d(n, j).start()
        for hf in range(2):
            ag_m(n, OWN, hf).start()

    def ag_step(n, *js):
        def f():
            for j in js:
                ag_u(n, j).wait_recv()
                if j + 2 < 7:
                    ag_u(n, j + 2).start()
                ag_d(n, j).wait_recv()
                if j + 2 < 7:
                    ag_d(n, j + 2).start()
                ag_m(n, AU[j // 2 + 1], j % 2).start()
                ag_m(n, AD[j // 2 + 1], 1 - j % 2).start()
        return f

    def ag_have(n, *ks):
        def f():
            for k in ks:
                for hf in range(2):
                    ag_m(n, k, hf).wait_recv()
        return f

    def ag_sent(n):
        for j in range(7):
            ag_u(n, j).wait_send()
            ag_d(n, j).wait_send()
        for k in range(8):
            for hf in range(2):
                ag_m(n, k, hf).wait_send()

    def rs_l(n, b, ch):
        return rcopy(ps.at[b, pl.ds(2 * ch, 2), 1], dr.at[b, pl.ds(2 * ch, 2)],
                     rx_s.at[n, ch], rx_r.at[n, ch], mate)

    def rs_u(n, b, j):
        return rcopy(ps.at[b, UP[(j + 1) // 2], 0, half(j % 2)], ru.at[b, j],
                     rs_s.at[n, 0, j], rs_r.at[n, 0, j], up)

    def rs_d(n, b, j):
        return rcopy(ps.at[b, DOWN[(j + 1) // 2], 0, half(1 - j % 2)], rd.at[b, j],
                     rs_s.at[n, 1, j], rs_r.at[n, 1, j], down)

    def rs_local(n, b, *chs):
        def f():
            for ch in chs:
                rs_l(n, b, ch).start()
        return f

    def rs_merge(n, b, *chs):
        def f():
            for ch in chs:
                rs_l(n, b, ch).wait_recv()
                for k in (2 * ch, 2 * ch + 1):
                    ps[b, k, 0] += dr[b, k]
        return f

    def rs_first(n, b):
        def f():
            rs_u(n, b, 0).start()
            rs_d(n, b, 0).start()
            rs_u(n, b, 1).start()
        return f

    def rs_second(n, b):
        def f():
            rs_d(n, b, 1).start()
        return f

    def rs_step(n, b, *js):
        def f():
            for j in js:
                k = (j + 3) // 2
                rs_u(n, b, j).wait_recv()
                ps[b, UP[k], 0, half(j % 2)] += ru[b, j]
                if j + 2 < 7:
                    rs_u(n, b, j + 2).start()
                rs_d(n, b, j).wait_recv()
                ps[b, DOWN[k], 0, half(1 - j % 2)] += rd[b, j]
                if j + 2 < 7:
                    rs_d(n, b, j + 2).start()
        return f

    def rs_sent(n, b):
        for j in range(7):
            rs_u(n, b, j).wait_send()
            rs_d(n, b, j).wait_send()
        for ch in range(4):
            rs_l(n, b, ch).wait_send()

    def token_loop(hooks, first, second):
        def at(it, p):
            for (i, q), fs in hooks.items():
                if q == p:
                    @pl.when(it == i)
                    def _():
                        for f in fs:
                            f()

        @pl.loop(0, 8)
        def _(it):
            e = it % 2
            ch = it // 2
            rows = pl.ds(pl.multiple_of(ch * R, R), R)
            at(it, 0)
            kept = first(ch, e, rows)
            if second is not None:
                at(it, 1)
                second(ch, e, rows, *kept)

    def gate(l, e, rows):
        return jnp.where(e == 0, gc_ref[rows, 2 * l:2 * l + 1], gc_ref[rows, 2 * l + 1:2 * l + 2])

    def rows_of(n, ch):
        return xg[n, pl.ds(2 * ch, 2)].reshape(R, -1)

    def put(b, ch, e, v):
        s = pl.ds(2 * ch, 2)
        ps[b, s] = jnp.where(e == 0, 0.0, ps[b, s]) + v.reshape(2, 2, T, v.shape[-1])

    def act(a1):
        sg = 1.0 / (1.0 + jnp.exp(-a1))
        return sg, a1 * sg

    def forward(l, n, b, ch, e, rows, a1s, a3s):
        g = gate(l, e, rows)
        u = rows_of(n, ch)
        a1 = _nn(u, w1[l, e])
        a3 = _nn(u, w3[l, e])
        sg, sl = act(a1)
        h = jnp.where(g >= 0, sl * a3, 0.0).astype(BF)
        a1s[...] = a1
        a3s[...] = a3
        hs[l, e, rows] = h
        put(b, ch, e, g * _nn(h, w2[l, e]).astype(BF).astype(F32))
        return ()

    def backward(l, nz, b, ch, e, rows, a1s, a3s):
        g = gate(l, e, rows)
        a1 = a1s[...]
        a3 = a3s[...]
        sg, sl = act(a1)
        h = hs[l, e, rows]
        r = _nt(rows_of(nz, ch), w2[l, e])
        dg = jnp.sum(h.astype(F32) * r, axis=1, keepdims=True)
        lane = lax.broadcasted_iota(jnp.int32, (R, 8), 1)
        dgc[rows, 0:8] = jnp.where(lane == 2 * l + e, dg, dgc[rows, 0:8])
        dh = g * r
        da3 = jnp.where(g >= 0, dh * sl, 0.0).astype(BF)
        da1 = jnp.where(g >= 0, dh * a3 * sg * (1.0 + a1 * (1.0 - sg)), 0.0).astype(BF)
        d1s[l, e, rows] = da1
        d3s[l, e, rows] = da3
        put(b, ch, e, (_nt(da1, w1[l, e]) + _nt(da3, w3[l, e])).astype(BF).astype(F32))
        return ()

    ag_start(0)
    gmsgs = []
    for k in range(8):
        q = (pos - REL[k] + 8) % 8
        for plane in range(2):
            if k == OWN and plane == 0:
                continue
            dev = _ring_ep(q, core + plane * (1 - 2 * core))
            c = rcopy(gts.at[pl.ds(dev * 8, 8)], gtr.at[pl.ds((k * 2 + plane) * 8, 8)],
                      g_s.at[k * 2 + plane], g_r.at[k * 2 + plane], dev)
            c.start()
            gmsgs.append(c)
    gtr[16 * OWN:16 * OWN + 8] = gts[pl.ds(pl.multiple_of(me * 8, 8), 8)]
    for c in wcopies[:3]:
        c.wait()
    for c in gmsgs:
        c.wait_recv()
    gct = gtr[...].T
    for b in range(16):
        gc_ref[b * T:(b + 1) * T, 0:8] = gct[0:T, b * 8:b * 8 + 8]

    token_loop({
        (0, 0): [ag_step(0, 0, 1), ag_have(0, 0, 1)],
        (1, 0): [ag_step(0, 2)],
        (2, 0): [ag_step(0, 3), ag_have(0, 2, 3), rs_local(0, 0, 0)],
        (3, 0): [ag_step(0, 4)],
        (4, 0): [ag_step(0, 5, 6), lambda: ag_start(1), ag_have(0, 4, 5), rs_local(0, 0, 1)],
        (6, 0): [rs_local(0, 0, 2), ag_have(0, 6, 7)],
        (7, 0): [rs_merge(0, 0, 2), rs_first(0, 0)],
    }, lambda ch, e, rows: forward(0, 0, 0, ch, e, rows, a1s.at[e, rows], a3s.at[e, rows]), None)
    rs_local(0, 0, 3)()
    rs_merge(0, 0, 0, 1, 3)()
    rs_second(0, 0)()
    for j in range(7):
        rs_step(0, 0, j)()
        ag_step(1, j)()
    xg[2, OWN, 0] = (x0_ref[...].astype(F32) + ps[0, OWN, 0]).astype(BF)
    ag_start(2)
    rs_sent(0, 0)
    for c in wcopies[3:]:
        c.wait()
    ag_have(1, *range(8))()

    token_loop({
        (0, 0): [ag_step(2, 0, 1), ag_have(2, 0, 1)],
        (0, 1): [ag_step(2, 2)],
        (1, 0): [ag_step(2, 3)],
        (1, 1): [ag_step(2, 4)],
        (2, 0): [ag_step(2, 5), ag_have(2, 2, 3), rs_local(2, 0, 0), rs_local(1, 1, 0)],
        (2, 1): [ag_step(2, 6)],
        (4, 0): [ag_have(2, 4, 5), rs_local(2, 0, 1), rs_local(1, 1, 1)],
        (6, 0): [rs_local(2, 0, 2), rs_local(1, 1, 2), ag_have(2, 6, 7)],
        (6, 1): [rs_merge(2, 0, 2), rs_first(2, 0), rs_merge(2, 0, 0, 1)],
        (7, 1): [rs_merge(1, 1, 2, 0, 1)],
    }, lambda ch, e, rows: forward(1, 2, 1, ch, e, rows, tmp1, tmp3),
        lambda ch, e, rows: backward(1, 1, 0, ch, e, rows, tmp1, tmp3))
    rs_local(2, 0, 3)()
    rs_local(1, 1, 3)()
    rs_merge(2, 0, 3)()
    rs_second(2, 0)()
    outs = []

    def out(src, dst, i):
        c = pltpu.make_async_copy(src, dst, osem.at[i])
        c.start()
        outs.append(c)
    for i, (s, d) in enumerate(((hs, h_o), (d1s, da1_o), (d3s, da3_o))):
        out(s.at[1], d.at[1], i)
    out(xg.at[0], xg_o.at[0], 3)
    out(xg.at[2], xg_o.at[1], 4)
    out(xg.at[1], zg_o.at[1], 5)
    rs_step(2, 0, *range(5))()
    rs_merge(1, 1, 3)()
    rs_step(2, 0, 5, 6)()
    xg[3, OWN, 0] = (dy_ref[...].astype(F32) + ps[0, OWN, 0]).astype(BF)
    ag_start(3)
    rs_sent(2, 0)

    token_loop({
        (0, 0): [ag_step(3, 0, 1), ag_have(3, 0, 1)],
        (1, 0): [ag_step(3, 2)],
        (2, 0): [ag_step(3, 3), ag_have(3, 2, 3), rs_local(3, 0, 0)],
        (3, 0): [ag_step(3, 4)],
        (4, 0): [ag_step(3, 5, 6), rs_first(1, 1), rs_second(1, 1), ag_have(3, 4, 5), rs_local(3, 0, 1)],
        (6, 0): [rs_local(3, 0, 2), ag_have(3, 6, 7)],
        (7, 0): [rs_merge(3, 0, 2), rs_first(3, 0), rs_step(1, 1, 0)],
    }, lambda ch, e, rows: backward(0, 3, 0, ch, e, rows, a1s.at[e, rows], a3s.at[e, rows]), None)
    rs_local(3, 0, 3)()
    rs_merge(3, 0, 0, 1, 3)()
    rs_second(3, 0)()
    out(xg.at[3], zg_o.at[0], 6)
    for i, (s, d) in enumerate(((hs, h_o), (d1s, da1_o), (d3s, da3_o))):
        out(s.at[0], d.at[0], 7 + i)

    dmsgs = []
    for k in range(8):
        t = dgc[k * 2 * T:(k + 1) * 2 * T].T[0:8]
        dgs[k * 16:k * 16 + 8] = t
        dgs[k * 16 + 8:k * 16 + 16] = pltpu.roll(t, T, 1)
        q = (pos + REL[k] + 8) % 8
        for plane in range(2):
            b = k * 2 + plane
            if k == OWN and plane == 0:
                continue
            dev = _ring_ep(q, core + plane * (1 - 2 * core))
            c = rcopy(dgs.at[pl.ds(b * 8, 8)], dgr_ref.at[pl.ds(me * 8, 8)], d_s.at[b], d_r.at[b], dev)
            c.start()
            dmsgs.append(c)
    dgr_ref[pl.ds(pl.multiple_of(me * 8, 8), 8)] = dgs[16 * OWN:16 * OWN + 8]

    for j in range(7):
        rs_step(3, 0, j)()
        if j < 6:
            rs_step(1, 1, j + 1)()
    dx0_ref[...] = (xg[3, OWN, 0].astype(F32) + ps[0, OWN, 0]).astype(BF)
    x2_ref[...] = (xg[2, OWN, 0].astype(F32) + ps[1, OWN, 0]).astype(BF)
    for c in dmsgs:
        c.wait_recv()
    for c in gmsgs + dmsgs:
        c.wait_send()
    for n in range(4):
        ag_sent(n)
    rs_sent(1, 1)
    rs_sent(3, 0)
    for c in outs:
        c.wait()


def _main(x0, dy, meta, ws):
    T, D = x0.shape
    EL, _, F = ws[0].shape
    N = 16 * T
    S = jax.ShapeDtypeStruct
    vm = pl.BlockSpec(memory_space=pltpu.VMEM)
    hb = pl.BlockSpec(memory_space=pl.ANY)
    dma = pltpu.SemaphoreType.DMA
    return pl.pallas_call(
        _main_kernel,
        out_shape=(S((T, D), BF), S((T, D), BF), S((128, 128), F32), S((N, 128), F32),
                   S((2, 8, 2, T, D), BF), S((2, 8, 2, T, D), BF),
                   S((2, EL, N, F), BF), S((2, EL, N, F), BF), S((2, EL, N, F), BF)),
        in_specs=[vm] * 3 + [hb] * 6,
        out_specs=(vm, vm, vm, vm) + (hb,) * 5,
        scratch_shapes=[
            pltpu.VMEM((2, EL, D, F), BF), pltpu.VMEM((2, EL, D, F), BF), pltpu.VMEM((2, EL, F, D), BF),
            pltpu.VMEM((4, 8, 2, T, D), BF),
            pltpu.VMEM((2, 8, 2, T, D), F32), pltpu.VMEM((2, 8, T, D), F32),
            pltpu.VMEM((2, 7, T // 2, D), F32), pltpu.VMEM((2, 7, T // 2, D), F32),
            pltpu.VMEM((EL, N, F), F32), pltpu.VMEM((EL, N, F), F32),
            pltpu.VMEM((2, EL, N, F), BF), pltpu.VMEM((2, EL, N, F), BF), pltpu.VMEM((2, EL, N, F), BF),
            pltpu.VMEM((128, 128), F32), pltpu.VMEM((128, 128), F32), pltpu.VMEM((N, 128), F32),
            pltpu.VMEM((128, 128), F32),
            pltpu.VMEM((4 * T, F), F32), pltpu.VMEM((4 * T, F), F32),
            dma((6,)), dma((4, 2, 7)), dma((4, 2, 7)), dma((4, 16)), dma((4, 16)),
            dma((4, 2, 7)), dma((4, 2, 7)), dma((4, 4)), dma((4, 4)),
            dma((16,)), dma((16,)), dma((16,)), dma((16,)), dma((10,)),
        ],
        compiler_params=pltpu.CompilerParams(collective_id=0, has_side_effects=True,
                                             vmem_limit_bytes=VMEM_LIMIT),
        name='moe',
    )(x0, dy, meta, *ws)


def _tn(a, b):
    return lax.dot_general(a, b, (((0,), (0,)), ((), ())), preferred_element_type=F32)


def _wgrad_kernel(x2_r, dx0_r, dgr, meta, gc, xg_h, zg_h, h_h, d1_h, d3_h,
                  x2_o, dx0_o, o1a, o3a, o2a, o1b, o3b, o2b, dga, dgb,
                  x, z, h, d1, d3, o1, o3, o2, isem, osem):
    T = x2_r.shape[0]
    ins = []
    for l in (1, 0):
        for i, (s, d) in enumerate(((xg_h, x), (d1_h, d1), (d3_h, d3), (zg_h, z), (h_h, h))):
            c = pltpu.make_async_copy(s.at[l], d.at[l], isem.at[l, i])
            c.start()
            ins.append(c)
    x2_o[...] = x2_r[...]
    dx0_o[...] = dx0_r[...]
    for l, o in ((0, dga), (1, dgb)):
        idx = meta[8 * l:8 * l + 8]
        acc = jnp.zeros((8, 128), F32)
        for i in range(16):
            for e in range(2):
                row = dgr[8 * i + 2 * l + e:8 * i + 2 * l + e + 1]
                acc = jnp.where(idx == float(2 * i + e), row, acc)
        o[...] = acc.T[0:T]
    outrefs = ((o1a, o3a, o2a), (o1b, o3b, o2b))

    def ocopy(l, i, e):
        return pltpu.make_async_copy((o1, o3, o2)[i].at[l, e], outrefs[l][i].at[e], osem.at[l, e, i])
    for n, l in enumerate((1, 0)):
        for c in ins[5 * n:5 * n + 5]:
            c.wait()

        @pl.loop(0, 2)
        def _(e):
            o1[l, e] = _tn(x[l], d1[l, e])
            ocopy(l, 0, e).start()
            o3[l, e] = _tn(x[l], d3[l, e])
            ocopy(l, 1, e).start()
            g = jnp.where(e == 0, gc[:, 2 * l:2 * l + 1], gc[:, 2 * l + 1:2 * l + 2])
            do = jnp.where(g >= 0, g * z[l].astype(F32), 0.0).astype(BF)
            o2[l, e] = _tn(h[l, e], do)
            ocopy(l, 2, e).start()
    for l in range(2):
        for e in range(2):
            for i in range(3):
                ocopy(l, i, e).wait()


def _wgrad(x2, dx0, dgr, meta, gc, xg, zg, h, d1, d3):
    T = x2.shape[0]
    _, N, D = xg.shape
    EL, F = h.shape[1], h.shape[3]
    S = jax.ShapeDtypeStruct
    vm = pl.BlockSpec(memory_space=pltpu.VMEM)
    hb = pl.BlockSpec(memory_space=pl.ANY)
    dma = pltpu.SemaphoreType.DMA
    up, dn = S((EL, D, F), F32), S((EL, F, D), F32)
    return pl.pallas_call(
        _wgrad_kernel,
        out_shape=(S((T, D), BF), S((T, D), BF), up, up, dn, up, up, dn, S((T, 8), F32), S((T, 8), F32)),
        in_specs=[vm] * 5 + [hb] * 5,
        out_specs=(vm, vm) + (hb,) * 6 + (vm, vm),
        scratch_shapes=[
            pltpu.VMEM((2, N, D), BF), pltpu.VMEM((2, N, D), BF), pltpu.VMEM((2, EL, N, F), BF),
            pltpu.VMEM((2, EL, N, F), BF), pltpu.VMEM((2, EL, N, F), BF),
            pltpu.VMEM((2, EL, D, F), F32), pltpu.VMEM((2, EL, D, F), F32), pltpu.VMEM((2, EL, F, D), F32),
            dma((2, 5)), dma((2, EL, 3)),
        ],
        compiler_params=pltpu.CompilerParams(vmem_limit_bytes=VMEM_LIMIT),
        name='wgrad',
    )(x2, dx0, dgr, meta, gc, xg, zg, h, d1, d3)


def solution(mesh):
    tok = P(('dp', 'ep'))
    wsp = P('ep')

    def body(x0, idx_a, g_a, idx_b, g_b, dy, *ws):
        T, D = x0.shape
        N = 16 * T
        meta = jnp.concatenate([idx_a.astype(F32), idx_b.astype(F32), g_a, g_b], axis=1).T
        meta = jnp.pad(meta, ((0, 0), (0, 128 - T)))
        x2, dx0, dgr, gc, xg, zg, h, d1, d3 = _main(x0, dy, meta, ws)
        return _wgrad(x2, dx0, dgr, meta, gc, xg.reshape(2, N, D), zg.reshape(2, N, D), h, d1, d3)

    return jax.shard_map(body, mesh=mesh,
                         in_specs=(tok,) * 6 + (wsp,) * 6,
                         out_specs=(tok,) * 10,
                         check_vma=False)
```

```python
import jax
import jax.numpy as jnp
from jax import lax
from jax.experimental import pallas as pl
from jax.experimental.pallas import tpu as pltpu
from jax.sharding import PartitionSpec as P

F32 = jnp.float32
BF = jnp.bfloat16
MESH = pl.DeviceIdType.MESH
VMEM_LIMIT = 67043328

REL = (-1, 1, -2, 2, -3, 3, 4, 0)
OWN = 7
UP = (6, 5, 3, 1, 7)
DOWN = (6, 4, 2, 0, 7)


def _ring_pos(ep):
    z, y = ep // 4, (ep // 2) % 2
    return z + y * (7 - 2 * z)


def _ring_ep(pos, core):
    y = pos // 4
    z = pos + y * (7 - 2 * pos)
    return z * 4 + y * 2 + core


def _nt(a, b):
    return lax.dot_general(a, b, (((1,), (1,)), ((), ())), preferred_element_type=F32)


def _nn(a, b):
    return jnp.dot(a, b, preferred_element_type=F32)


def _main_kernel(x0_ref, dy_ref, ia_ref, ib_ref, ga_ref, gb_ref, w1a_h, w3a_h, w2a_h, w1b_h, w3b_h, w2b_h,
                 x2_ref, dx0_ref, dgr_ref, gc_ref, xg_o, zg_o, h_o, da1_o, da3_o,
                 w1, w3, w2, xg, ps, dr, ru, rd, a1s, a3s, hs, d1s, d3s, gts, gtr, dgc, dgs, tmp1, tmp3,
                 wsem, ag_s, ag_r, ax_s, ax_r, rs_s, rs_r, rx_s, rx_r, g_s, g_r, d_s, d_r, osem):
    T = x0_ref.shape[0]
    H = T // 2
    R = 4 * T
    me = lax.axis_index('ep')
    core = me % 2
    pos = _ring_pos(me)
    up = _ring_ep((pos + 1) % 8, core)
    down = _ring_ep((pos + 7) % 8, core)
    mate = me + 1 - 2 * core

    wcopies = []
    for l, refs in enumerate(((w1a_h, w3a_h, w2a_h), (w1b_h, w3b_h, w2b_h))):
        for i, (src, dst) in enumerate(zip(refs, (w1, w3, w2))):
            c = pltpu.make_async_copy(src, dst.at[l], wsem.at[l * 3 + i])
            c.start()
            wcopies.append(c)

    bar = pltpu.get_barrier_semaphore()
    for i in range(1, 16):
        pl.semaphore_signal(bar, inc=1, device_id={'ep': (me + i) % 16}, device_id_type=MESH)
    xg[0, OWN, 0] = x0_ref[...]
    xg[1, OWN, 0] = dy_ref[...]
    gts[...] = jnp.full_like(gts, -1.0)
    for l, (ir, gr) in enumerate(((ia_ref, ga_ref), (ib_ref, gb_ref))):
        idx, gt = ir[...], gr[...]
        for i in range(16):
            for e in range(2):
                row = jnp.max(jnp.where(idx == 2 * i + e, gt, -1.0), axis=0, keepdims=True)
                gts[8 * i + 2 * l + e:8 * i + 2 * l + e + 1, 0:T] = row
    dgc[...] = jnp.zeros_like(dgc)
    pl.semaphore_wait(bar, 15)

    def rcopy(src, dst, ss, rs, dev):
        return pltpu.make_async_remote_copy(src_ref=src, dst_ref=dst, send_sem=ss, recv_sem=rs,
                                            device_id={'ep': dev}, device_id_type=MESH)

    def half(i):
        return pl.ds(i * H, H)

    pending = []

    AU, AD = (7, 0, 2, 4, 6), (7, 1, 3, 5, 6)

    def ag_u(n, j):
        i, h = j // 2, half(j % 2)
        return rcopy(xg.at[n, AU[i], 0, h], xg.at[n, AU[i + 1], 0, h], ag_s.at[n, 0, j], ag_r.at[n, 0, j], up)

    def ag_d(n, j):
        i, h = j // 2, half(1 - j % 2)
        return rcopy(xg.at[n, AD[i], 0, h], xg.at[n, AD[i + 1], 0, h], ag_s.at[n, 1, j], ag_r.at[n, 1, j], down)

    def ag_m(n, k, hf):
        return rcopy(xg.at[n, k, 0, half(hf)], xg.at[n, k, 1, half(hf)],
                     ax_s.at[n, k * 2 + hf], ax_r.at[n, k * 2 + hf], mate)

    def ag_start(n):
        for j in range(2):
            ag_u(n, j).start()
            ag_d(n, j).start()
        for hf in range(2):
            ag_m(n, OWN, hf).start()

    def ag_step(n, *js):
        def f():
            for j in js:
                ag_u(n, j).wait_recv()
                if j + 2 < 7:
                    ag_u(n, j + 2).start()
                ag_d(n, j).wait_recv()
                if j + 2 < 7:
                    ag_d(n, j + 2).start()
                ag_m(n, AU[j // 2 + 1], j % 2).start()
                ag_m(n, AD[j // 2 + 1], 1 - j % 2).start()
        return f

    def ag_have(n, *ks):
        def f():
            for k in ks:
                for hf in range(2):
                    ag_m(n, k, hf).wait_recv()
        return f

    def ag_sent(n):
        for j in range(7):
            ag_u(n, j).wait_send()
            ag_d(n, j).wait_send()
        for k in range(8):
            for hf in range(2):
                ag_m(n, k, hf).wait_send()

    def rs_l(n, b, ch):
        return rcopy(ps.at[b, pl.ds(2 * ch, 2), 1], dr.at[b, pl.ds(2 * ch, 2)],
                     rx_s.at[n, ch], rx_r.at[n, ch], mate)

    def rs_u(n, b, j):
        return rcopy(ps.at[b, UP[(j + 1) // 2], 0, half(j % 2)], ru.at[b, j],
                     rs_s.at[n, 0, j], rs_r.at[n, 0, j], up)

    def rs_d(n, b, j):
        return rcopy(ps.at[b, DOWN[(j + 1) // 2], 0, half(1 - j % 2)], rd.at[b, j],
                     rs_s.at[n, 1, j], rs_r.at[n, 1, j], down)

    def rs_local(n, b, *chs):
        def f():
            for ch in chs:
                rs_l(n, b, ch).start()
        return f

    def rs_merge(n, b, *chs):
        def f():
            for ch in chs:
                rs_l(n, b, ch).wait_recv()
                for k in (2 * ch, 2 * ch + 1):
                    ps[b, k, 0] += dr[b, k]
        return f

    def rs_first(n, b):
        def f():
            rs_u(n, b, 1).start()
            rs_d(n, b, 1).start()
        return f

    def rs_second(n, b):
        def f():
            rs_u(n, b, 0).start()
            rs_d(n, b, 0).start()
        return f

    def rs_step(n, b, *js):
        def f():
            for j in js:
                k = (j + 3) // 2
                rs_u(n, b, j).wait_recv()
                ps[b, UP[k], 0, half(j % 2)] += ru[b, j]
                if j + 2 < 7:
                    rs_u(n, b, j + 2).start()
                rs_d(n, b, j).wait_recv()
                ps[b, DOWN[k], 0, half(1 - j % 2)] += rd[b, j]
                if j + 2 < 7:
                    rs_d(n, b, j + 2).start()
        return f

    def rs_sent(n, b):
        for j in range(7):
            rs_u(n, b, j).wait_send()
            rs_d(n, b, j).wait_send()
        for ch in range(4):
            rs_l(n, b, ch).wait_send()

    def token_loop(hooks, *stages):
        ns = len(stages)

        @pl.loop(0, 8 * ns)
        def _(it):
            for i, fs in hooks.items():
                @pl.when(it == i)
                def _():
                    for f in fs:
                        f()
            ch = it // (2 * ns)
            e = it % 2
            rows = pl.ds(pl.multiple_of(ch * R, R), R)
            if ns == 1:
                stages[0](ch, e, rows)
            else:
                for k in range(ns):
                    @pl.when((it // 2) % ns == k)
                    def _():
                        stages[k](ch, e, rows)

    def gate(l, e, rows):
        return jnp.where(e == 0, gc_ref[rows, 2 * l:2 * l + 1], gc_ref[rows, 2 * l + 1:2 * l + 2])

    def rows_of(n, ch):
        return xg[n, pl.ds(2 * ch, 2)].reshape(R, -1)

    def put(b, ch, e, v):
        s = pl.ds(2 * ch, 2)
        ps[b, s] = jnp.where(e == 0, 0.0, ps[b, s]) + v.reshape(2, 2, T, v.shape[-1])

    def act(a1):
        sg = 1.0 / (1.0 + jnp.exp(-a1))
        return sg, a1 * sg

    def forward(l, n, b, ch, e, rows, a1s, a3s):
        g = gate(l, e, rows)
        u = rows_of(n, ch)
        a1 = _nn(u, w1[l, e])
        a3 = _nn(u, w3[l, e])
        sg, sl = act(a1)
        h = jnp.where(g >= 0, sl * a3, 0.0).astype(BF)
        a1s[...] = a1
        a3s[...] = a3
        hs[l, e, rows] = h
        put(b, ch, e, g * _nn(h, w2[l, e]).astype(BF).astype(F32))
        return ()

    def backward(l, nz, b, ch, e, rows, a1s, a3s):
        g = gate(l, e, rows)
        a1 = a1s[...]
        a3 = a3s[...]
        sg, sl = act(a1)
        h = hs[l, e, rows]
        r = _nt(rows_of(nz, ch), w2[l, e])
        dg = jnp.sum(h.astype(F32) * r, axis=1, keepdims=True)
        lane = lax.broadcasted_iota(jnp.int32, (R, 8), 1)
        dgc[rows, 0:8] = jnp.where(lane == 2 * l + e, dg, dgc[rows, 0:8])
        dh = g * r
        da3 = jnp.where(g >= 0, dh * sl, 0.0).astype(BF)
        da1 = jnp.where(g >= 0, dh * a3 * sg * (1.0 + a1 * (1.0 - sg)), 0.0).astype(BF)
        d1s[l, e, rows] = da1
        d3s[l, e, rows] = da3
        put(b, ch, e, (_nt(da1, w1[l, e]) + _nt(da3, w3[l, e])).astype(BF).astype(F32))
        return ()

    ag_start(0)
    gmsgs = []
    for k in range(8):
        q = (pos - REL[k] + 8) % 8
        for plane in range(2):
            if k == OWN and plane == 0:
                continue
            dev = _ring_ep(q, core + plane * (1 - 2 * core))
            c = rcopy(gts.at[pl.ds(dev * 8, 8)], gtr.at[pl.ds((k * 2 + plane) * 8, 8)],
                      g_s.at[k * 2 + plane], g_r.at[k * 2 + plane], dev)
            c.start()
            gmsgs.append(c)
    gtr[16 * OWN:16 * OWN + 8] = gts[pl.ds(pl.multiple_of(me * 8, 8), 8)]
    for c in wcopies[:3]:
        c.wait()
    for c in gmsgs:
        c.wait_recv()
    gct = gtr[...].T
    for b in range(16):
        gc_ref[b * T:(b + 1) * T, 0:8] = gct[0:T, b * 8:b * 8 + 8]

    token_loop({
        0: [ag_step(0, 0, 1), ag_have(0, 0, 1)],
        1: [ag_step(0, 2)],
        2: [ag_step(0, 3), ag_have(0, 2, 3), rs_local(0, 0, 0)],
        3: [ag_step(0, 4)],
        4: [ag_step(0, 5), lambda: ag_start(1), ag_have(0, 4, 5)],
        5: [ag_step(0, 6), rs_local(0, 0, 1)],
        6: [rs_local(0, 0, 2), ag_have(0, 6, 7)],
        7: [rs_merge(0, 0, 2), rs_first(0, 0), ag_step(1, 0, 1)],
    }, lambda ch, e, rows: forward(0, 0, 0, ch, e, rows, a1s.at[e, rows], a3s.at[e, rows]))
    rs_local(0, 0, 3)()
    rs_merge(0, 0, 0, 1, 3)()
    rs_second(0, 0)()
    rs_step(0, 0, 1, 0, 3, 2, 5, 4)()
    ag_step(1, 2, 3)()
    rs_step(0, 0, 6)()
    xg[2, OWN, 0] = (x0_ref[...].astype(F32) + ps[0, OWN, 0]).astype(BF)
    ag_start(2)
    rs_sent(0, 0)
    for c in wcopies[3:]:
        c.wait()

    token_loop({
        0: [ag_step(2, 0, 1), ag_have(2, 0, 1)],
        1: [ag_step(2, 2), ag_step(1, 4)],
        2: [ag_step(2, 3), ag_step(1, 5), ag_have(1, 0, 1)],
        3: [ag_step(2, 4), ag_step(1, 6)],
        4: [ag_step(2, 5), ag_have(2, 2, 3), rs_local(2, 0, 0), rs_local(1, 1, 0)],
        5: [ag_step(2, 6)],
        6: [ag_have(1, 2, 3)],
        8: [ag_have(2, 4, 5), rs_local(2, 0, 1), rs_local(1, 1, 1)],
        10: [rs_local(1, 1, 2), ag_have(1, 4, 5), rs_merge(1, 1, 0, 1)],
        11: [rs_merge(1, 1, 2), rs_first(1, 1)],
        12: [rs_local(2, 0, 2), ag_have(2, 6, 7)],
        13: [rs_merge(2, 0, 2), rs_first(2, 0), rs_merge(2, 0, 0, 1)],
        14: [rs_local(1, 1, 3), ag_have(1, 6, 7)],
        15: [rs_merge(1, 1, 3), rs_second(1, 1)],
    }, lambda ch, e, rows: forward(1, 2, 1, ch, e, rows, tmp1.at[e], tmp3.at[e]),
        lambda ch, e, rows: backward(1, 1, 0, ch, e, rows, tmp1.at[e], tmp3.at[e]))
    rs_local(2, 0, 3)()
    outs = []

    def out(src, dst, i):
        c = pltpu.make_async_copy(src, dst, osem.at[i])
        c.start()
        outs.append(c)
    for i, (sr, ds) in enumerate(((hs, h_o), (d1s, da1_o), (d3s, da3_o))):
        out(sr.at[1], ds.at[1], i)
    out(xg.at[0], xg_o.at[0], 3)
    out(xg.at[2], xg_o.at[1], 4)
    out(xg.at[1], zg_o.at[1], 5)
    rs_merge(2, 0, 3)()
    rs_second(2, 0)()
    rs_step(2, 0, 1, 0, 3, 2, 5, 4)()
    rs_step(1, 1, 1)()
    rs_step(2, 0, 6)()
    xg[3, OWN, 0] = (dy_ref[...].astype(F32) + ps[0, OWN, 0]).astype(BF)
    ag_start(3)
    rs_sent(2, 0)

    token_loop({
        0: [ag_step(3, 0, 1), ag_have(3, 0, 1)],
        1: [ag_step(3, 2)],
        2: [ag_step(3, 3), ag_have(3, 2, 3), rs_local(3, 0, 0)],
        3: [ag_step(3, 4)],
        4: [ag_step(3, 5), rs_step(1, 1, 0), ag_have(3, 4, 5)],
        5: [ag_step(3, 6), rs_step(1, 1, 3), rs_local(3, 0, 1)],
        6: [rs_local(3, 0, 2), ag_have(3, 6, 7)],
        7: [rs_merge(3, 0, 2), rs_first(3, 0)],
    }, lambda ch, e, rows: backward(0, 3, 0, ch, e, rows, a1s.at[e, rows], a3s.at[e, rows]))
    rs_local(3, 0, 3)()
    out(xg.at[3], zg_o.at[0], 6)
    for i, (sr, ds) in enumerate(((hs, h_o), (d1s, da1_o), (d3s, da3_o))):
        out(sr.at[0], ds.at[0], 7 + i)
    rs_merge(3, 0, 0, 1, 3)()
    rs_second(3, 0)()

    dmsgs = []
    for k in range(8):
        t = dgc[k * 2 * T:(k + 1) * 2 * T].T[0:8]
        dgs[k * 16:k * 16 + 8] = t
        dgs[k * 16 + 8:k * 16 + 16] = pltpu.roll(t, T, 1)
        q = (pos + REL[k] + 8) % 8
        for plane in range(2):
            b = k * 2 + plane
            if k == OWN and plane == 0:
                continue
            dev = _ring_ep(q, core + plane * (1 - 2 * core))
            c = rcopy(dgs.at[pl.ds(b * 8, 8)], dgr_ref.at[pl.ds(me * 8, 8)], d_s.at[b], d_r.at[b], dev)
            c.start()
            dmsgs.append(c)
    dgr_ref[pl.ds(pl.multiple_of(me * 8, 8), 8)] = dgs[16 * OWN:16 * OWN + 8]

    rs_step(3, 0, 1, 0)()
    rs_step(1, 1, 2)()
    rs_step(3, 0, 3, 2)()
    rs_step(1, 1, 5, 4)()
    rs_step(3, 0, 5, 4)()
    rs_step(1, 1, 6)()
    rs_step(3, 0, 6)()
    dx0_ref[...] = (xg[3, OWN, 0].astype(F32) + ps[0, OWN, 0]).astype(BF)
    x2_ref[...] = (xg[2, OWN, 0].astype(F32) + ps[1, OWN, 0]).astype(BF)
    for c in dmsgs:
        c.wait_recv()
    for c in gmsgs + dmsgs:
        c.wait_send()
    for n in range(4):
        ag_sent(n)
    rs_sent(1, 1)
    rs_sent(3, 0)
    for c in outs:
        c.wait()


def _main(x0, dy, meta, ws):
    T, D = x0.shape
    EL, _, F = ws[0].shape
    N = 16 * T
    S = jax.ShapeDtypeStruct
    vm = pl.BlockSpec(memory_space=pltpu.VMEM)
    hb = pl.BlockSpec(memory_space=pl.ANY)
    dma = pltpu.SemaphoreType.DMA
    return pl.pallas_call(
        _main_kernel,
        out_shape=(S((T, D), BF), S((T, D), BF), S((128, 128), F32), S((N, 128), F32),
                   S((2, 8, 2, T, D), BF), S((2, 8, 2, T, D), BF),
                   S((2, EL, N, F), BF), S((2, EL, N, F), BF), S((2, EL, N, F), BF)),
        in_specs=[vm] * 6 + [hb] * 6,
        out_specs=(vm, vm, vm, vm) + (hb,) * 5,
        scratch_shapes=[
            pltpu.VMEM((2, EL, D, F), BF), pltpu.VMEM((2, EL, D, F), BF), pltpu.VMEM((2, EL, F, D), BF),
            pltpu.VMEM((4, 8, 2, T, D), BF),
            pltpu.VMEM((2, 8, 2, T, D), F32), pltpu.VMEM((2, 8, T, D), F32),
            pltpu.VMEM((2, 7, T // 2, D), F32), pltpu.VMEM((2, 7, T // 2, D), F32),
            pltpu.VMEM((EL, N, F), F32), pltpu.VMEM((EL, N, F), F32),
            pltpu.VMEM((2, EL, N, F), BF), pltpu.VMEM((2, EL, N, F), BF), pltpu.VMEM((2, EL, N, F), BF),
            pltpu.VMEM((128, 128), F32), pltpu.VMEM((128, 128), F32), pltpu.VMEM((N, 128), F32),
            pltpu.VMEM((128, 128), F32),
            pltpu.VMEM((EL, 4 * T, F), F32), pltpu.VMEM((EL, 4 * T, F), F32),
            dma((6,)), dma((4, 2, 7)), dma((4, 2, 7)), dma((4, 16)), dma((4, 16)),
            dma((4, 2, 7)), dma((4, 2, 7)), dma((4, 4)), dma((4, 4)),
            dma((16,)), dma((16,)), dma((16,)), dma((16,)), dma((10,)),
        ],
        compiler_params=pltpu.CompilerParams(collective_id=0, has_side_effects=True,
                                             vmem_limit_bytes=VMEM_LIMIT),
        name='moe',
    )(x0, dy, *meta, *ws)


def _tn(a, b):
    return lax.dot_general(a, b, (((0,), (0,)), ((), ())), preferred_element_type=F32)


def _wgrad_kernel(x2_r, dx0_r, dgr, ia_ref, ib_ref, gc, xg_h, zg_h, h_h, d1_h, d3_h,
                  x2_o, dx0_o, o1a, o3a, o2a, o1b, o3b, o2b, dga, dgb,
                  x, z, h, d1, d3, o1, o3, o2, isem, osem):
    T = x2_r.shape[0]
    ins = []
    for l in (1, 0):
        for i, (s, d) in enumerate(((xg_h, x), (d1_h, d1), (d3_h, d3), (zg_h, z), (h_h, h))):
            c = pltpu.make_async_copy(s.at[l], d.at[l], isem.at[l, i])
            c.start()
            ins.append(c)
    x2_o[...] = x2_r[...]
    dx0_o[...] = dx0_r[...]
    for l, ir, o in ((0, ia_ref, dga), (1, ib_ref, dgb)):
        idx = ir[...]
        acc = jnp.zeros((8, T), F32)
        for i in range(16):
            for e in range(2):
                row = dgr[8 * i + 2 * l + e:8 * i + 2 * l + e + 1, 0:T]
                acc = jnp.where(idx == 2 * i + e, row, acc)
        o[...] = acc
    outrefs = ((o1a, o3a, o2a), (o1b, o3b, o2b))

    def ocopy(l, i, e):
        return pltpu.make_async_copy((o1, o3, o2)[i].at[l, e], outrefs[l][i].at[e], osem.at[l, e, i])
    for n, l in enumerate((1, 0)):
        for c in ins[5 * n:5 * n + 3]:
            c.wait()

        @pl.loop(0, 2)
        def _(e):
            o1[l, e] = _tn(x[l], d1[l, e])
            ocopy(l, 0, e).start()
            o3[l, e] = _tn(x[l], d3[l, e])
            ocopy(l, 1, e).start()
        for c in ins[5 * n + 3:5 * n + 5]:
            c.wait()

        @pl.loop(0, 2)
        def _(e):
            g = jnp.where(e == 0, gc[:, 2 * l:2 * l + 1], gc[:, 2 * l + 1:2 * l + 2])
            do = jnp.where(g >= 0, g * z[l].astype(F32), 0.0).astype(BF)
            o2[l, e] = _tn(h[l, e], do)
            ocopy(l, 2, e).start()
    for l in range(2):
        for e in range(2):
            for i in range(3):
                ocopy(l, i, e).wait()


def _wgrad(x2, dx0, dgr, meta, gc, xg, zg, h, d1, d3):
    T = x2.shape[0]
    _, N, D = xg.shape
    EL, F = h.shape[1], h.shape[3]
    S = jax.ShapeDtypeStruct
    vm = pl.BlockSpec(memory_space=pltpu.VMEM)
    hb = pl.BlockSpec(memory_space=pl.ANY)
    dma = pltpu.SemaphoreType.DMA
    up, dn = S((EL, D, F), F32), S((EL, F, D), F32)
    return pl.pallas_call(
        _wgrad_kernel,
        out_shape=(S((T, D), BF), S((T, D), BF), up, up, dn, up, up, dn, S((8, T), F32), S((8, T), F32)),
        in_specs=[vm] * 6 + [hb] * 5,
        out_specs=(vm, vm) + (hb,) * 6 + (vm, vm),
        scratch_shapes=[
            pltpu.VMEM((2, N, D), BF), pltpu.VMEM((2, N, D), BF), pltpu.VMEM((2, EL, N, F), BF),
            pltpu.VMEM((2, EL, N, F), BF), pltpu.VMEM((2, EL, N, F), BF),
            pltpu.VMEM((2, EL, D, F), F32), pltpu.VMEM((2, EL, D, F), F32), pltpu.VMEM((2, EL, F, D), F32),
            dma((2, 5)), dma((2, EL, 3)),
        ],
        compiler_params=pltpu.CompilerParams(vmem_limit_bytes=VMEM_LIMIT),
        name='wgrad',
    )(x2, dx0, dgr, *meta, gc, xg, zg, h, d1, d3)


def solution(mesh):
    tok = P(('dp', 'ep'))
    wsp = P('ep')

    def body(x0, idx_a, g_a, idx_b, g_b, dy, *ws):
        T, D = x0.shape
        N = 16 * T
        ids = (idx_a.T, idx_b.T)
        x2, dx0, dgr, gc, xg, zg, h, d1, d3 = _main(x0, dy, ids + (g_a.T, g_b.T), ws)
        r = _wgrad(x2, dx0, dgr, ids, gc, xg.reshape(2, N, D), zg.reshape(2, N, D), h, d1, d3)
        return tuple(r[:8]) + (r[8].T, r[9].T)

    return jax.shard_map(body, mesh=mesh,
                         in_specs=(tok,) * 6 + (wsp,) * 6,
                         out_specs=(tok,) * 10,
                         check_vma=False)
```

```python
import jax
import jax.numpy as jnp
from jax import lax
from jax.experimental import pallas as pl
from jax.experimental.pallas import tpu as pltpu
from jax.sharding import PartitionSpec as P

F32 = jnp.float32
BF = jnp.bfloat16
MESH = pl.DeviceIdType.MESH
VMEM_LIMIT = 67043328

REL = (-1, 1, -2, 2, -3, 3, 4, 0)
OWN = 7
UP = (6, 5, 3, 1, 7)
DOWN = (6, 4, 2, 0, 7)


def _ring_pos(ep):
    z, y = ep // 4, (ep // 2) % 2
    return z + y * (7 - 2 * z)


def _ring_ep(pos, core):
    y = pos // 4
    z = pos + y * (7 - 2 * pos)
    return z * 4 + y * 2 + core


def _nt(a, b):
    return lax.dot_general(a, b, (((1,), (1,)), ((), ())), preferred_element_type=F32)


def _nn(a, b):
    return jnp.dot(a, b, preferred_element_type=F32)


def _main_kernel(x0_ref, dy_ref, ia_ref, ib_ref, ga_ref, gb_ref, w1a_h, w3a_h, w2a_h, w1b_h, w3b_h, w2b_h,
                 x2_ref, dx0_ref, dgr_ref, gc_ref, xg_o, zg_o, h_o, da1_o, da3_o,
                 w1, w3, w2, xg, ps, dr, ru, rd, a1s, a3s, hs, d1s, d3s, gq, gtr, dgc, dgs, tmp1, tmp3,
                 wsem, gq_s, gq_r, gx_s, gx_r, ag_s, ag_r, ax_s, ax_r, rs_s, rs_r, rx_s, rx_r, d_s, d_r, osem):
    T = x0_ref.shape[0]
    H = T // 2
    R = 4 * T
    xin = [pltpu.make_async_copy(r, xg.at[n, OWN, 0], osem.at[n])
           for n, r in enumerate((x0_ref, dy_ref))]
    for c in xin:
        c.start()
    me = lax.axis_index('ep')
    core = me % 2
    pos = _ring_pos(me)
    up = _ring_ep((pos + 1) % 8, core)
    down = _ring_ep((pos + 7) % 8, core)
    mate = me + 1 - 2 * core

    wcopies = []
    for l, refs in enumerate(((w1a_h, w3a_h, w2a_h), (w1b_h, w3b_h, w2b_h))):
        for i, (src, dst) in enumerate(zip(refs, (w1, w3, w2))):
            c = pltpu.make_async_copy(src, dst.at[l], wsem.at[l * 3 + i])
            c.start()
            wcopies.append(c)

    bar = pltpu.get_barrier_semaphore()
    for dev in (up, down, mate):
        pl.semaphore_signal(bar, inc=1, device_id={'ep': dev}, device_id_type=MESH)
    for l, (ir, gr) in enumerate(((ia_ref, ga_ref), (ib_ref, gb_ref))):
        gq[OWN, 0, 8 * l:8 * l + 8, 0:T] = ir[...].astype(F32)
        gq[OWN, 0, 8 * l:8 * l + 8, T:2 * T] = gr[...]
    gtr[...] = jnp.full_like(gtr, -1.0)
    dgc[...] = jnp.zeros_like(dgc)
    for c in xin:
        c.wait()
    pl.semaphore_wait(bar, 3)

    def rcopy(src, dst, ss, rs, dev):
        return pltpu.make_async_remote_copy(src_ref=src, dst_ref=dst, send_sem=ss, recv_sem=rs,
                                            device_id={'ep': dev}, device_id_type=MESH)

    Q = H // 2

    def half(i):
        return pl.ds(i * H, H)

    def quarter(i, q):
        return pl.ds(i * H + q * Q, Q)

    pending = []

    AU, AD = (7, 0, 2, 4, 6), (7, 1, 3, 5, 6)

    def ag_u(n, j, q):
        i, h, m = j // 2, quarter(j % 2, q), 2 * j + q
        return rcopy(xg.at[n, AU[i], 0, h], xg.at[n, AU[i + 1], 0, h], ag_s.at[n, 0, m], ag_r.at[n, 0, m], up)

    def ag_d(n, j, q):
        i, h, m = j // 2, quarter(1 - j % 2, q), 2 * j + q
        return rcopy(xg.at[n, AD[i], 0, h], xg.at[n, AD[i + 1], 0, h], ag_s.at[n, 1, m], ag_r.at[n, 1, m], down)

    def ag_m(n, k, hf):
        return rcopy(xg.at[n, k, 0, half(hf)], xg.at[n, k, 1, half(hf)],
                     ax_s.at[n, k * 2 + hf], ax_r.at[n, k * 2 + hf], mate)

    def gq_u(h):
        return rcopy(gq.at[AU[h], 0], gq.at[AU[h + 1], 0], gq_s.at[0, h], gq_r.at[0, h], up)

    def gq_d(h):
        return rcopy(gq.at[AD[h], 0], gq.at[AD[h + 1], 0], gq_s.at[1, h], gq_r.at[1, h], down)

    def gq_m(k):
        return rcopy(gq.at[k, 0], gq.at[k, 1], gx_s.at[k], gx_r.at[k], mate)

    def gq_step(h):
        def f():
            gq_u(h).wait_recv()
            if h < 3:
                gq_u(h + 1).start()
            gq_m(AU[h + 1]).start()
            if h < 3:
                gq_d(h).wait_recv()
                if h < 2:
                    gq_d(h + 1).start()
                gq_m(AD[h + 1]).start()
        return f

    def gates(ch):
        def f():
            for k in (2 * ch, 2 * ch + 1):
                gq_m(k).wait_recv()
                for plane in range(2):
                    for l in range(2):
                        t = gq[k, plane, 8 * l:8 * l + 8]
                        gt = pltpu.roll(t, T, 1)
                        for e in range(2):
                            row = 8 * (2 * k + plane) + 2 * l + e
                            mine = (2 * me + e).astype(F32)
                            gtr[row:row + 1] = jnp.max(jnp.where(t == mine, gt, -1.0), axis=0, keepdims=True)
            gct = gtr[...].T
            for b in range(4 * ch, 4 * ch + 4):
                gc_ref[b * T:(b + 1) * T, 0:8] = gct[0:T, b * 8:b * 8 + 8]
        return f

    def ag_start(n):
        for j in range(2):
            for q in range(2):
                ag_u(n, j, q).start()
                ag_d(n, j, q).start()
        for hf in range(2):
            ag_m(n, OWN, hf).start()

    def ag_step(n, *js):
        def f():
            for j in js:
                for q in range(2):
                    ag_u(n, j, q).wait_recv()
                    if j + 2 < 7:
                        ag_u(n, j + 2, q).start()
                    ag_d(n, j, q).wait_recv()
                    if j + 2 < 7:
                        ag_d(n, j + 2, q).start()
                ag_m(n, AU[j // 2 + 1], j % 2).start()
                ag_m(n, AD[j // 2 + 1], 1 - j % 2).start()
        return f

    def ag_have(n, *ks):
        def f():
            for k in ks:
                for hf in range(2):
                    ag_m(n, k, hf).wait_recv()
        return f

    def ag_sent(n):
        for j in range(7):
            for q in range(2):
                ag_u(n, j, q).wait_send()
                ag_d(n, j, q).wait_send()
        for k in range(8):
            for hf in range(2):
                ag_m(n, k, hf).wait_send()

    def rs_l(n, b, ch):
        return rcopy(ps.at[b, pl.ds(2 * ch, 2), 1], dr.at[b, pl.ds(2 * ch, 2)],
                     rx_s.at[n, ch], rx_r.at[n, ch], mate)

    def rs_u(n, b, j, q):
        m = 2 * j + q
        return rcopy(ps.at[b, UP[(j + 1) // 2], 0, quarter(j % 2, q)], ru.at[b, j, quarter(0, q)],
                     rs_s.at[n, 0, m], rs_r.at[n, 0, m], up)

    def rs_d(n, b, j, q):
        m = 2 * j + q
        return rcopy(ps.at[b, DOWN[(j + 1) // 2], 0, quarter(1 - j % 2, q)], rd.at[b, j, quarter(0, q)],
                     rs_s.at[n, 1, m], rs_r.at[n, 1, m], down)

    def rs_local(n, b, *chs):
        def f():
            for ch in chs:
                rs_l(n, b, ch).start()
        return f

    def rs_merge(n, b, *chs):
        def f():
            for ch in chs:
                rs_l(n, b, ch).wait_recv()
                for k in (2 * ch, 2 * ch + 1):
                    ps[b, k, 0] += dr[b, k]
        return f

    def rs_first(n, b):
        def f():
            for q in range(2):
                rs_u(n, b, 1, q).start()
                rs_d(n, b, 1, q).start()
        return f

    def rs_second(n, b):
        def f():
            for q in range(2):
                rs_u(n, b, 0, q).start()
                rs_d(n, b, 0, q).start()
        return f

    def rs_step(n, b, *js):
        def f():
            for j in js:
                k = (j + 3) // 2
                for q in range(2):
                    rs_u(n, b, j, q).wait_recv()
                    ps[b, UP[k], 0, quarter(j % 2, q)] += ru[b, j, quarter(0, q)]
                    if j + 2 < 7:
                        rs_u(n, b, j + 2, q).start()
                    rs_d(n, b, j, q).wait_recv()
                    ps[b, DOWN[k], 0, quarter(1 - j % 2, q)] += rd[b, j, quarter(0, q)]
                    if j + 2 < 7:
                        rs_d(n, b, j + 2, q).start()
        return f

    def rs_sent(n, b):
        for j in range(7):
            for q in range(2):
                rs_u(n, b, j, q).wait_send()
                rs_d(n, b, j, q).wait_send()
        for ch in range(4):
            rs_l(n, b, ch).wait_send()

    def token_loop(hooks, *stages):
        ns = len(stages)

        @pl.loop(0, 8 * ns)
        def _(it):
            for i, fs in hooks.items():
                @pl.when(it == i)
                def _():
                    for f in fs:
                        f()
            ch = it // (2 * ns)
            e = it % 2
            rows = pl.ds(pl.multiple_of(ch * R, R), R)
            if ns == 1:
                stages[0](ch, e, rows)
            else:
                for k in range(ns):
                    @pl.when((it // 2) % ns == k)
                    def _():
                        stages[k](ch, e, rows)

    def gate(l, e, rows):
        return jnp.where(e == 0, gc_ref[rows, 2 * l:2 * l + 1], gc_ref[rows, 2 * l + 1:2 * l + 2])

    def rows_of(n, ch):
        return xg[n, pl.ds(2 * ch, 2)].reshape(R, -1)

    def put(b, ch, e, v):
        s = pl.ds(2 * ch, 2)
        ps[b, s] = jnp.where(e == 0, 0.0, ps[b, s]) + v.reshape(2, 2, T, v.shape[-1])

    def act(a1):
        sg = 1.0 / (1.0 + jnp.exp(-a1))
        return sg, a1 * sg

    def forward(l, n, b, ch, e, rows, a1s, a3s):
        g = gate(l, e, rows)
        u = rows_of(n, ch)
        a1 = _nn(u, w1[l, e])
        a3 = _nn(u, w3[l, e])
        sg, sl = act(a1)
        h = jnp.where(g >= 0, sl * a3, 0.0).astype(BF)
        a1s[...] = a1
        a3s[...] = a3
        hs[l, e, rows] = h
        put(b, ch, e, g * _nn(h, w2[l, e]).astype(BF).astype(F32))
        return ()

    def backward(l, nz, b, ch, e, rows, a1s, a3s):
        g = gate(l, e, rows)
        a1 = a1s[...]
        a3 = a3s[...]
        sg, sl = act(a1)
        h = hs[l, e, rows]
        r = _nt(rows_of(nz, ch), w2[l, e])
        dg = jnp.sum(h.astype(F32) * r, axis=1, keepdims=True)
        lane = lax.broadcasted_iota(jnp.int32, (R, 8), 1)
        dgc[rows, 0:8] = jnp.where(lane == 2 * l + e, dg, dgc[rows, 0:8])
        dh = g * r
        da3 = jnp.where(g >= 0, dh * sl, 0.0).astype(BF)
        da1 = jnp.where(g >= 0, dh * a3 * sg * (1.0 + a1 * (1.0 - sg)), 0.0).astype(BF)
        d1s[l, e, rows] = da1
        d3s[l, e, rows] = da3
        put(b, ch, e, (_nt(da1, w1[l, e]) + _nt(da3, w3[l, e])).astype(BF).astype(F32))
        return ()

    gq_u(0).start()
    gq_d(0).start()
    gq_m(OWN).start()
    ag_start(0)
    for c in wcopies[:3]:
        c.wait()
    token_loop({
        0: [gq_step(0), ag_step(0, 0, 1), gates(0), ag_have(0, 0, 1)],
        1: [gq_step(1), ag_step(0, 2)],
        2: [ag_step(0, 3), gates(1), ag_have(0, 2, 3), rs_local(0, 0, 0)],
        3: [gq_step(2), ag_step(0, 4)],
        4: [ag_step(0, 5), lambda: ag_start(1), gates(2), ag_have(0, 4, 5)],
        5: [gq_step(3), ag_step(0, 6), rs_local(0, 0, 1)],
        6: [rs_local(0, 0, 2), gates(3), ag_have(0, 6, 7)],
        7: [rs_merge(0, 0, 2), rs_first(0, 0), ag_step(1, 0, 1)],
    }, lambda ch, e, rows: forward(0, 0, 0, ch, e, rows, a1s.at[e, rows], a3s.at[e, rows]))
    rs_local(0, 0, 3)()
    rs_merge(0, 0, 0, 1, 3)()
    rs_second(0, 0)()
    rs_step(0, 0, 1, 0, 3, 2, 5, 4)()
    ag_step(1, 2, 3)()
    rs_step(0, 0, 6)()
    xg[2, OWN, 0] = (xg[0, OWN, 0].astype(F32) + ps[0, OWN, 0]).astype(BF)
    ag_start(2)
    rs_sent(0, 0)
    for c in wcopies[3:]:
        c.wait()

    token_loop({
        0: [ag_step(2, 0, 1), ag_have(2, 0, 1)],
        1: [ag_step(2, 2), ag_step(1, 4)],
        2: [ag_step(2, 3), ag_step(1, 5), ag_have(1, 0, 1)],
        3: [ag_step(2, 4), ag_step(1, 6)],
        4: [ag_step(2, 5), ag_have(2, 2, 3), rs_local(2, 0, 0), rs_local(1, 1, 0)],
        5: [ag_step(2, 6)],
        6: [ag_have(1, 2, 3)],
        8: [ag_have(2, 4, 5), rs_local(2, 0, 1), rs_local(1, 1, 1)],
        10: [rs_local(1, 1, 2), ag_have(1, 4, 5), rs_merge(1, 1, 0, 1)],
        11: [rs_merge(1, 1, 2), rs_first(1, 1)],
        12: [rs_local(2, 0, 2), ag_have(2, 6, 7)],
        13: [rs_merge(2, 0, 2), rs_first(2, 0), rs_merge(2, 0, 0, 1)],
        14: [rs_local(1, 1, 3), ag_have(1, 6, 7)],
        15: [rs_merge(1, 1, 3), rs_second(1, 1)],
    }, lambda ch, e, rows: forward(1, 2, 1, ch, e, rows, tmp1.at[e], tmp3.at[e]),
        lambda ch, e, rows: backward(1, 1, 0, ch, e, rows, tmp1.at[e], tmp3.at[e]))
    rs_local(2, 0, 3)()
    outs = []

    def out(src, dst, i):
        c = pltpu.make_async_copy(src, dst, osem.at[i])
        c.start()
        outs.append(c)
    for i, (sr, ds) in enumerate(((hs, h_o), (d1s, da1_o), (d3s, da3_o))):
        out(sr.at[1], ds.at[1], i)
    out(xg.at[0], xg_o.at[0], 3)
    out(xg.at[2], xg_o.at[1], 4)
    out(xg.at[1], zg_o.at[1], 5)
    rs_merge(2, 0, 3)()
    rs_second(2, 0)()
    rs_step(2, 0, 1, 0, 3, 2, 5, 4)()
    rs_step(1, 1, 1)()
    rs_step(2, 0, 6)()
    xg[3, OWN, 0] = (xg[1, OWN, 0].astype(F32) + ps[0, OWN, 0]).astype(BF)
    ag_start(3)
    rs_sent(2, 0)

    token_loop({
        0: [ag_step(3, 0, 1), ag_have(3, 0, 1)],
        1: [ag_step(3, 2)],
        2: [ag_step(3, 3), ag_have(3, 2, 3), rs_local(3, 0, 0)],
        3: [ag_step(3, 4)],
        4: [ag_step(3, 5), rs_step(1, 1, 0), ag_have(3, 4, 5)],
        5: [ag_step(3, 6), rs_step(1, 1, 3), rs_local(3, 0, 1)],
        6: [rs_local(3, 0, 2), ag_have(3, 6, 7)],
        7: [rs_merge(3, 0, 2), rs_first(3, 0)],
    }, lambda ch, e, rows: backward(0, 3, 0, ch, e, rows, a1s.at[e, rows], a3s.at[e, rows]))
    rs_local(3, 0, 3)()
    out(xg.at[3], zg_o.at[0], 6)
    for i, (sr, ds) in enumerate(((hs, h_o), (d1s, da1_o), (d3s, da3_o))):
        out(sr.at[0], ds.at[0], 7 + i)
    rs_merge(3, 0, 0, 1, 3)()
    rs_second(3, 0)()

    dmsgs = []
    for k in range(8):
        t = dgc[k * 2 * T:(k + 1) * 2 * T].T[0:8]
        dgs[k * 16:k * 16 + 8] = t
        dgs[k * 16 + 8:k * 16 + 16] = pltpu.roll(t, T, 1)
        q = (pos + REL[k] + 8) % 8
        for plane in range(2):
            b = k * 2 + plane
            if k == OWN and plane == 0:
                continue
            dev = _ring_ep(q, core + plane * (1 - 2 * core))
            c = rcopy(dgs.at[pl.ds(b * 8, 8)], dgr_ref.at[pl.ds(me * 8, 8)], d_s.at[b], d_r.at[b], dev)
            c.start()
            dmsgs.append(c)
    dgr_ref[pl.ds(pl.multiple_of(me * 8, 8), 8)] = dgs[16 * OWN:16 * OWN + 8]

    rs_step(3, 0, 1, 0)()
    rs_step(1, 1, 2)()
    rs_step(3, 0, 3, 2)()
    rs_step(1, 1, 5, 4)()
    rs_step(3, 0, 5, 4)()
    rs_step(1, 1, 6)()
    rs_step(3, 0, 6)()
    dx0_ref[...] = (xg[3, OWN, 0].astype(F32) + ps[0, OWN, 0]).astype(BF)
    x2_ref[...] = (xg[2, OWN, 0].astype(F32) + ps[1, OWN, 0]).astype(BF)
    for c in dmsgs:
        c.wait_recv()
    for c in dmsgs + [gq_u(h) for h in range(4)] + [gq_d(h) for h in range(3)] + [gq_m(k) for k in range(8)]:
        c.wait_send()
    for n in range(4):
        ag_sent(n)
    rs_sent(1, 1)
    rs_sent(3, 0)
    for c in outs:
        c.wait()


def _main(x0, dy, meta, ws):
    T, D = x0.shape
    EL, _, F = ws[0].shape
    N = 16 * T
    S = jax.ShapeDtypeStruct
    vm = pl.BlockSpec(memory_space=pltpu.VMEM)
    hb = pl.BlockSpec(memory_space=pl.ANY)
    dma = pltpu.SemaphoreType.DMA
    return pl.pallas_call(
        _main_kernel,
        out_shape=(S((T, D), BF), S((T, D), BF), S((128, 128), F32), S((N, 128), F32),
                   S((2, 8, 2, T, D), BF), S((2, 8, 2, T, D), BF),
                   S((2, EL, N, F), BF), S((2, EL, N, F), BF), S((2, EL, N, F), BF)),
        in_specs=[hb] * 2 + [vm] * 4 + [hb] * 6,
        out_specs=(vm, vm, vm, vm) + (hb,) * 5,
        scratch_shapes=[
            pltpu.VMEM((2, EL, D, F), BF), pltpu.VMEM((2, EL, D, F), BF), pltpu.VMEM((2, EL, F, D), BF),
            pltpu.VMEM((4, 8, 2, T, D), BF),
            pltpu.VMEM((2, 8, 2, T, D), F32), pltpu.VMEM((2, 8, T, D), F32),
            pltpu.VMEM((2, 7, T // 2, D), F32), pltpu.VMEM((2, 7, T // 2, D), F32),
            pltpu.VMEM((EL, N, F), F32), pltpu.VMEM((EL, N, F), F32),
            pltpu.VMEM((2, EL, N, F), BF), pltpu.VMEM((2, EL, N, F), BF), pltpu.VMEM((2, EL, N, F), BF),
            pltpu.VMEM((8, 2, 16, 128), F32), pltpu.VMEM((128, 128), F32), pltpu.VMEM((N, 128), F32),
            pltpu.VMEM((128, 128), F32),
            pltpu.VMEM((EL, 4 * T, F), F32), pltpu.VMEM((EL, 4 * T, F), F32),
            dma((6,)), dma((2, 4)), dma((2, 4)), dma((8,)), dma((8,)),
            dma((4, 2, 14)), dma((4, 2, 14)), dma((4, 16)), dma((4, 16)),
            dma((4, 2, 14)), dma((4, 2, 14)), dma((4, 4)), dma((4, 4)),
            dma((16,)), dma((16,)), dma((10,)),
        ],
        compiler_params=pltpu.CompilerParams(collective_id=0, has_side_effects=True,
                                             vmem_limit_bytes=VMEM_LIMIT),
        name='moe',
    )(x0, dy, *meta, *ws)


def _tn(a, b):
    return lax.dot_general(a, b, (((0,), (0,)), ((), ())), preferred_element_type=F32)


def _wgrad_kernel(x2_r, dx0_r, dgr, ia_ref, ib_ref, gc, xg_h, zg_h, h_h, d1_h, d3_h,
                  x2_o, dx0_o, o1a, o3a, o2a, o1b, o3b, o2b, dga, dgb,
                  x, z, h, d1, d3, o1, o3, o2, isem, osem):
    T = x2_r.shape[0]
    ins = []
    for l in (1, 0):
        for i, (s, d) in enumerate(((xg_h, x), (d1_h, d1), (d3_h, d3), (zg_h, z), (h_h, h))):
            c = pltpu.make_async_copy(s.at[l], d.at[l], isem.at[l, i])
            c.start()
            ins.append(c)
    x2_o[...] = x2_r[...]
    dx0_o[...] = dx0_r[...]
    for l, ir, o in ((0, ia_ref, dga), (1, ib_ref, dgb)):
        idx = ir[...]
        acc = jnp.zeros((8, T), F32)
        for i in range(16):
            for e in range(2):
                row = dgr[8 * i + 2 * l + e:8 * i + 2 * l + e + 1, 0:T]
                acc = jnp.where(idx == 2 * i + e, row, acc)
        o[...] = acc
    outrefs = ((o1a, o3a, o2a), (o1b, o3b, o2b))

    def ocopy(l, i, e):
        return pltpu.make_async_copy((o1, o3, o2)[i].at[l, e], outrefs[l][i].at[e], osem.at[l, e, i])
    for n, l in enumerate((1, 0)):
        for c in ins[5 * n:5 * n + 3]:
            c.wait()

        @pl.loop(0, 2)
        def _(e):
            o1[l, e] = _tn(x[l], d1[l, e])
            ocopy(l, 0, e).start()
            o3[l, e] = _tn(x[l], d3[l, e])
            ocopy(l, 1, e).start()
        for c in ins[5 * n + 3:5 * n + 5]:
            c.wait()

        @pl.loop(0, 2)
        def _(e):
            g = jnp.where(e == 0, gc[:, 2 * l:2 * l + 1], gc[:, 2 * l + 1:2 * l + 2])
            do = jnp.where(g >= 0, g * z[l].astype(F32), 0.0).astype(BF)
            o2[l, e] = _tn(h[l, e], do)
            ocopy(l, 2, e).start()
    for l in range(2):
        for e in range(2):
            for i in range(3):
                ocopy(l, i, e).wait()


def _wgrad(x2, dx0, dgr, meta, gc, xg, zg, h, d1, d3):
    T = x2.shape[0]
    _, N, D = xg.shape
    EL, F = h.shape[1], h.shape[3]
    S = jax.ShapeDtypeStruct
    vm = pl.BlockSpec(memory_space=pltpu.VMEM)
    hb = pl.BlockSpec(memory_space=pl.ANY)
    dma = pltpu.SemaphoreType.DMA
    up, dn = S((EL, D, F), F32), S((EL, F, D), F32)
    return pl.pallas_call(
        _wgrad_kernel,
        out_shape=(S((T, D), BF), S((T, D), BF), up, up, dn, up, up, dn, S((8, T), F32), S((8, T), F32)),
        in_specs=[vm] * 6 + [hb] * 5,
        out_specs=(vm, vm) + (hb,) * 6 + (vm, vm),
        scratch_shapes=[
            pltpu.VMEM((2, N, D), BF), pltpu.VMEM((2, N, D), BF), pltpu.VMEM((2, EL, N, F), BF),
            pltpu.VMEM((2, EL, N, F), BF), pltpu.VMEM((2, EL, N, F), BF),
            pltpu.VMEM((2, EL, D, F), F32), pltpu.VMEM((2, EL, D, F), F32), pltpu.VMEM((2, EL, F, D), F32),
            dma((2, 5)), dma((2, EL, 3)),
        ],
        compiler_params=pltpu.CompilerParams(vmem_limit_bytes=VMEM_LIMIT),
        name='wgrad',
    )(x2, dx0, dgr, *meta, gc, xg, zg, h, d1, d3)


def solution(mesh):
    tok = P(('dp', 'ep'))
    wsp = P('ep')

    def body(x0, idx_a, g_a, idx_b, g_b, dy, *ws):
        T, D = x0.shape
        N = 16 * T
        ids = (idx_a.T, idx_b.T)
        x2, dx0, dgr, gc, xg, zg, h, d1, d3 = _main(x0, dy, ids + (g_a.T, g_b.T), ws)
        r = _wgrad(x2, dx0, dgr, ids, gc, xg.reshape(2, N, D), zg.reshape(2, N, D), h, d1, d3)
        return tuple(r[:8]) + (r[8].T, r[9].T)

    return jax.shard_map(body, mesh=mesh,
                         in_specs=(tok,) * 6 + (wsp,) * 6,
                         out_specs=(tok,) * 10,
                         check_vma=False)
```

```python
import jax
import jax.numpy as jnp
from jax import lax
from jax.experimental import pallas as pl
from jax.experimental.pallas import tpu as pltpu
from jax.sharding import PartitionSpec as P

F32 = jnp.float32
BF = jnp.bfloat16
MESH = pl.DeviceIdType.MESH
VMEM_LIMIT = 67043328

REL = (-1, 1, -2, 2, -3, 3, 4, 0)
OWN = 7
UP = (6, 5, 3, 1, 7)
DOWN = (6, 4, 2, 0, 7)


def _ring_pos(ep):
    z, y = ep // 4, (ep // 2) % 2
    return z + y * (7 - 2 * z)


def _ring_ep(pos, core):
    y = pos // 4
    z = pos + y * (7 - 2 * pos)
    return z * 4 + y * 2 + core


def _nt(a, b):
    return lax.dot_general(a, b, (((1,), (1,)), ((), ())), preferred_element_type=F32)


def _nn(a, b):
    return jnp.dot(a, b, preferred_element_type=F32)


def _main_kernel(x0_ref, dy_ref, ia_ref, ib_ref, ga_ref, gb_ref, w1a_h, w3a_h, w2a_h, w1b_h, w3b_h, w2b_h,
                 x2_ref, dx0_ref, dgr_ref, gc_ref, xg_o, zg_o, h_o, d13_o,
                 w13, w2, xg, ps, dr, ru, rd, a13s, hs, d13s, gq, gtr, dgc, dgs, tmp,
                 wsem, gq_s, gq_r, gx_s, gx_r, ag_s, ag_r, ax_s, ax_r, rs_s, rs_r, rx_s, rx_r, d_s, d_r, osem):
    T = x0_ref.shape[0]
    H = T // 2
    F = w2.shape[2]
    R = 4 * T
    xin = [pltpu.make_async_copy(r, xg.at[n, OWN, 0], osem.at[n])
           for n, r in enumerate((x0_ref, dy_ref))]
    for c in xin:
        c.start()
    me = lax.axis_index('ep')
    core = me % 2
    pos = _ring_pos(me)
    up = _ring_ep((pos + 1) % 8, core)
    down = _ring_ep((pos + 7) % 8, core)
    mate = me + 1 - 2 * core

    wcopies = []
    for l, refs in enumerate(((w1a_h, w3a_h, w2a_h), (w1b_h, w3b_h, w2b_h))):
        for i, src in enumerate(refs):
            dst = w2.at[l] if i == 2 else w13.at[l, :, :, pl.ds(i * F, F)]
            c = pltpu.make_async_copy(src, dst, wsem.at[l * 3 + i])
            c.start()
            wcopies.append(c)

    bar = pltpu.get_barrier_semaphore()
    for dev in (up, down, mate):
        pl.semaphore_signal(bar, inc=1, device_id={'ep': dev}, device_id_type=MESH)
    for l, (ir, gr) in enumerate(((ia_ref, ga_ref), (ib_ref, gb_ref))):
        gq[OWN, 0, 8 * l:8 * l + 8, 0:T] = ir[...].astype(F32)
        gq[OWN, 0, 8 * l:8 * l + 8, T:2 * T] = gr[...]
    gtr[...] = jnp.full_like(gtr, -1.0)
    dgc[...] = jnp.zeros_like(dgc)
    for c in xin:
        c.wait()
    pl.semaphore_wait(bar, 3)

    def rcopy(src, dst, ss, rs, dev):
        return pltpu.make_async_remote_copy(src_ref=src, dst_ref=dst, send_sem=ss, recv_sem=rs,
                                            device_id={'ep': dev}, device_id_type=MESH)

    Q = H // 2

    def half(i):
        return pl.ds(i * H, H)

    def quarter(i, q):
        return pl.ds(i * H + q * Q, Q)

    AGSET = (0, 1, 0, 0)

    AU, AD = (7, 0, 2, 4, 6), (7, 1, 3, 5, 6)

    def ag_u(n, j, q):
        i, h, m = j // 2, quarter(j % 2, q), 2 * j + q
        return rcopy(xg.at[n, AU[i], 0, h], xg.at[n, AU[i + 1], 0, h], ag_s.at[AGSET[n], 0], ag_r.at[AGSET[n], 0, m], up)

    def ag_d(n, j, q):
        i, h, m = j // 2, quarter(1 - j % 2, q), 2 * j + q
        return rcopy(xg.at[n, AD[i], 0, h], xg.at[n, AD[i + 1], 0, h], ag_s.at[AGSET[n], 1], ag_r.at[AGSET[n], 1, m], down)

    def ag_m(n, k, hf):
        return rcopy(xg.at[n, k, 0, half(hf)], xg.at[n, k, 1, half(hf)],
                     ax_s.at[AGSET[n]], ax_r.at[AGSET[n], k * 2 + hf], mate)

    def gq_u(h):
        return rcopy(gq.at[AU[h], 0], gq.at[AU[h + 1], 0], gq_s.at[0], gq_r.at[0, h], up)

    def gq_d(h):
        return rcopy(gq.at[AD[h], 0], gq.at[AD[h + 1], 0], gq_s.at[1], gq_r.at[1, h], down)

    def gq_m(k):
        return rcopy(gq.at[k, 0], gq.at[k, 1], gx_s.at[0], gx_r.at[k], mate)

    def gq_step(h):
        def f():
            gq_u(h).wait_recv()
            if h < 3:
                gq_u(h + 1).start()
            gq_m(AU[h + 1]).start()
            if h < 3:
                gq_d(h).wait_recv()
                if h < 2:
                    gq_d(h + 1).start()
                gq_m(AD[h + 1]).start()
        return f

    def gates(ch):
        def f():
            for k in (2 * ch, 2 * ch + 1):
                gq_m(k).wait_recv()
                for plane in range(2):
                    for l in range(2):
                        t = gq[k, plane, 8 * l:8 * l + 8]
                        gt = pltpu.roll(t, T, 1)
                        for e in range(2):
                            row = 8 * (2 * k + plane) + 2 * l + e
                            mine = (2 * me + e).astype(F32)
                            gtr[row:row + 1] = jnp.max(jnp.where(t == mine, gt, -1.0), axis=0, keepdims=True)
            gct = gtr[...].T
            for b in range(4 * ch, 4 * ch + 4):
                gc_ref[b * T:(b + 1) * T, 0:8] = gct[0:T, b * 8:b * 8 + 8]
        return f

    def ag_start(n):
        for j in range(2):
            for q in range(2):
                ag_u(n, j, q).start()
                ag_d(n, j, q).start()
        for hf in range(2):
            ag_m(n, OWN, hf).start()

    def ag_step(n, *js):
        def f():
            for j in js:
                for q in range(2):
                    ag_u(n, j, q).wait_recv()
                    if j + 2 < 7:
                        ag_u(n, j + 2, q).start()
                    ag_d(n, j, q).wait_recv()
                    if j + 2 < 7:
                        ag_d(n, j + 2, q).start()
                ag_m(n, AU[j // 2 + 1], j % 2).start()
                ag_m(n, AD[j // 2 + 1], 1 - j % 2).start()
        return f

    def ag_have(n, *ks):
        def f():
            for k in ks:
                for hf in range(2):
                    ag_m(n, k, hf).wait_recv()
        return f

    def sent(ref, sem):
        pltpu.make_async_copy(ref, ref, sem).wait()

    def ag_sent(n):
        for d in range(2):
            sent(xg.at[n, pl.ds(0, 7), 0, half(0)], ag_s.at[AGSET[n], d])
        sent(xg.at[n, :, 0], ax_s.at[AGSET[n]])

    def rs_l(n, b, ch):
        return rcopy(ps.at[b, pl.ds(2 * ch, 2), 1], dr.at[b, pl.ds(2 * ch, 2)],
                     rx_s.at[b], rx_r.at[b, ch], mate)

    def rs_u(n, b, j, q):
        m = 2 * j + q
        return rcopy(ps.at[b, UP[(j + 1) // 2], 0, quarter(j % 2, q)], ru.at[b, j, quarter(0, q)],
                     rs_s.at[b, 0], rs_r.at[b, 0, m], up)

    def rs_d(n, b, j, q):
        m = 2 * j + q
        return rcopy(ps.at[b, DOWN[(j + 1) // 2], 0, quarter(1 - j % 2, q)], rd.at[b, j, quarter(0, q)],
                     rs_s.at[b, 1], rs_r.at[b, 1, m], down)

    def rs_local(n, b, *chs):
        def f():
            for ch in chs:
                rs_l(n, b, ch).start()
        return f

    def rs_merge(n, b, *chs):
        def f():
            for ch in chs:
                rs_l(n, b, ch).wait_recv()
                for k in (2 * ch, 2 * ch + 1):
                    ps[b, k, 0] += dr[b, k]
        return f

    def rs_first(n, b):
        def f():
            for q in range(2):
                rs_u(n, b, 1, q).start()
                rs_d(n, b, 1, q).start()
        return f

    def rs_second(n, b):
        def f():
            for q in range(2):
                rs_u(n, b, 0, q).start()
                rs_d(n, b, 0, q).start()
        return f

    def rs_step(n, b, *js):
        def f():
            for j in js:
                k = (j + 3) // 2
                for q in range(2):
                    rs_u(n, b, j, q).wait_recv()
                    ps[b, UP[k], 0, quarter(j % 2, q)] += ru[b, j, quarter(0, q)]
                    if j + 2 < 7:
                        rs_u(n, b, j + 2, q).start()
                    rs_d(n, b, j, q).wait_recv()
                    ps[b, DOWN[k], 0, quarter(1 - j % 2, q)] += rd[b, j, quarter(0, q)]
                    if j + 2 < 7:
                        rs_d(n, b, j + 2, q).start()
        return f

    def rs_sent(n, b):
        for d in range(2):
            sent(ps.at[b, pl.ds(0, 7), 0, half(0)], rs_s.at[b, d])
        sent(ps.at[b, :, 1], rx_s.at[b])

    def token_loop(hooks, *stages):
        ns = len(stages)

        @pl.loop(0, 8 * ns)
        def _(it):
            for i, fs in hooks.items():
                @pl.when(it == i)
                def _():
                    for f in fs:
                        f()
            ch = it // (2 * ns)
            e = it % 2
            rows = pl.ds(pl.multiple_of(ch * R, R), R)
            if ns == 1:
                stages[0](ch, e, rows)
            else:
                for k in range(ns):
                    @pl.when((it // 2) % ns == k)
                    def _():
                        stages[k](ch, e, rows)

    def gate(l, e, rows):
        return jnp.where(e == 0, gc_ref[rows, 2 * l:2 * l + 1], gc_ref[rows, 2 * l + 1:2 * l + 2])

    def rows_of(n, ch):
        return xg[n, pl.ds(2 * ch, 2)].reshape(R, -1)

    def put(b, ch, e, v):
        s = pl.ds(2 * ch, 2)
        ps[b, s] = jnp.where(e == 0, 0.0, ps[b, s]) + v.reshape(2, 2, T, v.shape[-1])

    def act(a1):
        sg = 1.0 / (1.0 + jnp.exp(-a1))
        return sg, a1 * sg

    def forward(l, n, b, ch, e, rows, a13s):
        g = gate(l, e, rows)
        a13 = _nn(rows_of(n, ch), w13[l, e])
        a13s[...] = a13
        sg, sl = act(a13[:, :F])
        h = jnp.where(g >= 0, sl * a13[:, F:], 0.0).astype(BF)
        hs[l, e, rows] = h
        put(b, ch, e, g * _nn(h, w2[l, e]).astype(BF).astype(F32))

    def backward(l, nz, b, ch, e, rows, a13s):
        g = gate(l, e, rows)
        a1 = a13s[:, :F]
        a3 = a13s[:, F:]
        sg, sl = act(a1)
        h = hs[l, e, rows]
        r = _nt(rows_of(nz, ch), w2[l, e])
        dg = jnp.sum(h.astype(F32) * r, axis=1, keepdims=True)
        lane = lax.broadcasted_iota(jnp.int32, (R, 8), 1)
        dgc[rows, 0:8] = jnp.where(lane == 2 * l + e, dg, dgc[rows, 0:8])
        dh = g * r
        da3 = jnp.where(g >= 0, dh * sl, 0.0).astype(BF)
        da1 = jnp.where(g >= 0, dh * a3 * sg * (1.0 + a1 * (1.0 - sg)), 0.0).astype(BF)
        d13s[l, e, rows, 0:F] = da1
        d13s[l, e, rows, F:2 * F] = da3
        put(b, ch, e, _nt(d13s[l, e, rows], w13[l, e]).astype(BF).astype(F32))

    gq_u(0).start()
    gq_d(0).start()
    gq_m(OWN).start()
    ag_start(0)
    for c in wcopies[:3]:
        c.wait()
    token_loop({
        0: [gq_step(0), ag_step(0, 0, 1), gates(0), ag_have(0, 0, 1)],
        1: [gq_step(1), ag_step(0, 2)],
        2: [ag_step(0, 3), gates(1), ag_have(0, 2, 3), rs_local(0, 0, 0)],
        3: [gq_step(2), ag_step(0, 4)],
        4: [ag_step(0, 5), lambda: ag_start(1), gates(2), ag_have(0, 4, 5)],
        5: [gq_step(3), ag_step(0, 6), rs_local(0, 0, 1)],
        6: [rs_local(0, 0, 2), gates(3), ag_have(0, 6, 7)],
        7: [rs_merge(0, 0, 2), rs_first(0, 0), ag_step(1, 0, 1)],
    }, lambda ch, e, rows: forward(0, 0, 0, ch, e, rows, a13s.at[e, rows]))
    rs_local(0, 0, 3)()
    rs_merge(0, 0, 0, 1, 3)()
    rs_second(0, 0)()
    rs_step(0, 0, 1, 0, 3, 2, 5, 4)()
    ag_step(1, 2, 3)()
    rs_step(0, 0, 6)()
    xg[2, OWN, 0] = (xg[0, OWN, 0].astype(F32) + ps[0, OWN, 0]).astype(BF)
    ag_sent(0)
    ag_start(2)
    rs_sent(0, 0)
    for c in wcopies[3:]:
        c.wait()

    token_loop({
        0: [ag_step(2, 0, 1), ag_have(2, 0, 1)],
        1: [ag_step(2, 2), ag_step(1, 4)],
        2: [ag_step(2, 3), ag_step(1, 5), ag_have(1, 0, 1)],
        3: [ag_step(2, 4), ag_step(1, 6)],
        4: [ag_step(2, 5), ag_have(2, 2, 3), rs_local(2, 0, 0), rs_local(1, 1, 0)],
        5: [ag_step(2, 6)],
        6: [ag_have(1, 2, 3)],
        8: [ag_have(2, 4, 5), rs_local(2, 0, 1), rs_local(1, 1, 1)],
        10: [rs_local(1, 1, 2), ag_have(1, 4, 5), rs_merge(1, 1, 0, 1)],
        11: [rs_merge(1, 1, 2), rs_first(1, 1)],
        12: [rs_local(2, 0, 2), ag_have(2, 6, 7)],
        13: [rs_merge(2, 0, 2), rs_first(2, 0), rs_merge(2, 0, 0, 1)],
        14: [rs_local(1, 1, 3), ag_have(1, 6, 7)],
        15: [rs_merge(1, 1, 3), rs_second(1, 1)],
    }, lambda ch, e, rows: forward(1, 2, 1, ch, e, rows, tmp.at[e]),
        lambda ch, e, rows: backward(1, 1, 0, ch, e, rows, tmp.at[e]))
    rs_local(2, 0, 3)()
    outs = []

    def out(src, dst, i):
        c = pltpu.make_async_copy(src, dst, osem.at[i])
        c.start()
        outs.append(c)
    for i, (sr, ds) in enumerate(((hs, h_o), (d13s, d13_o))):
        out(sr.at[1], ds.at[1], i)
    out(xg.at[0], xg_o.at[0], 3)
    out(xg.at[2], xg_o.at[1], 4)
    out(xg.at[1], zg_o.at[1], 5)
    rs_merge(2, 0, 3)()
    rs_second(2, 0)()
    rs_step(2, 0, 1, 0, 3, 2, 5, 4)()
    rs_step(1, 1, 1)()
    rs_step(2, 0, 6)()
    xg[3, OWN, 0] = (xg[1, OWN, 0].astype(F32) + ps[0, OWN, 0]).astype(BF)
    ag_sent(2)
    ag_start(3)
    rs_sent(2, 0)

    token_loop({
        0: [ag_step(3, 0, 1), ag_have(3, 0, 1)],
        1: [ag_step(3, 2)],
        2: [ag_step(3, 3), ag_have(3, 2, 3), rs_local(3, 0, 0)],
        3: [ag_step(3, 4)],
        4: [ag_step(3, 5), rs_step(1, 1, 0), ag_have(3, 4, 5)],
        5: [ag_step(3, 6), rs_step(1, 1, 3), rs_local(3, 0, 1)],
        6: [rs_local(3, 0, 2), ag_have(3, 6, 7)],
        7: [rs_merge(3, 0, 2), rs_first(3, 0)],
    }, lambda ch, e, rows: backward(0, 3, 0, ch, e, rows, a13s.at[e, rows]))
    rs_local(3, 0, 3)()
    out(xg.at[3], zg_o.at[0], 6)
    for i, (sr, ds) in enumerate(((hs, h_o), (d13s, d13_o))):
        out(sr.at[0], ds.at[0], 7 + i)
    rs_merge(3, 0, 0, 1, 3)()
    rs_second(3, 0)()

    for k in range(8):
        t = dgc[k * 2 * T:(k + 1) * 2 * T].T[0:8]
        dgs[k * 16:k * 16 + 8] = t
        dgs[k * 16 + 8:k * 16 + 16] = pltpu.roll(t, T, 1)
        q = (pos + REL[k] + 8) % 8
        for plane in range(2):
            b = k * 2 + plane
            if k == OWN and plane == 0:
                continue
            dev = _ring_ep(q, core + plane * (1 - 2 * core))
            c = rcopy(dgs.at[pl.ds(b * 8, 8)], dgr_ref.at[pl.ds(me * 8, 8)], d_s.at[0], d_r.at[0], dev)
            c.start()
    dgr_ref[pl.ds(pl.multiple_of(me * 8, 8), 8)] = dgs[16 * OWN:16 * OWN + 8]

    rs_step(3, 0, 1, 0)()
    rs_step(1, 1, 2)()
    rs_step(3, 0, 3, 2)()
    rs_step(1, 1, 5, 4)()
    rs_step(3, 0, 5, 4)()
    rs_step(1, 1, 6)()
    rs_step(3, 0, 6)()
    dx0_ref[...] = (xg[3, OWN, 0].astype(F32) + ps[0, OWN, 0]).astype(BF)
    x2_ref[...] = (xg[2, OWN, 0].astype(F32) + ps[1, OWN, 0]).astype(BF)
    sent(dgs.at[pl.ds(0, 120)], d_r.at[0])
    sent(dgs.at[pl.ds(0, 120)], d_s.at[0])
    sent(gq.at[pl.ds(0, 4), 0], gq_s.at[0])
    sent(gq.at[pl.ds(0, 3), 0], gq_s.at[1])
    sent(gq.at[:, 0], gx_s.at[0])
    for n in (1, 3):
        ag_sent(n)
    rs_sent(1, 1)
    rs_sent(3, 0)
    for c in outs:
        c.wait()


def _main(x0, dy, meta, ws):
    T, D = x0.shape
    EL, _, F = ws[0].shape
    N = 16 * T
    S = jax.ShapeDtypeStruct
    vm = pl.BlockSpec(memory_space=pltpu.VMEM)
    hb = pl.BlockSpec(memory_space=pl.ANY)
    dma = pltpu.SemaphoreType.DMA
    return pl.pallas_call(
        _main_kernel,
        out_shape=(S((T, D), BF), S((T, D), BF), S((128, 128), F32), S((N, 128), F32),
                   S((2, 8, 2, T, D), BF), S((2, 8, 2, T, D), BF),
                   S((2, EL, N, F), BF), S((2, EL, N, 2 * F), BF)),
        in_specs=[hb] * 2 + [vm] * 4 + [hb] * 6,
        out_specs=(vm, vm, vm, vm) + (hb,) * 4,
        scratch_shapes=[
            pltpu.VMEM((2, EL, D, 2 * F), BF), pltpu.VMEM((2, EL, F, D), BF),
            pltpu.VMEM((4, 8, 2, T, D), BF),
            pltpu.VMEM((2, 8, 2, T, D), F32), pltpu.VMEM((2, 8, T, D), F32),
            pltpu.VMEM((2, 7, T // 2, D), F32), pltpu.VMEM((2, 7, T // 2, D), F32),
            pltpu.VMEM((EL, N, 2 * F), F32),
            pltpu.VMEM((2, EL, N, F), BF), pltpu.VMEM((2, EL, N, 2 * F), BF),
            pltpu.VMEM((8, 2, 16, 128), F32), pltpu.VMEM((128, 128), F32), pltpu.VMEM((N, 128), F32),
            pltpu.VMEM((128, 128), F32),
            pltpu.VMEM((EL, 4 * T, 2 * F), F32),
            dma((6,)), dma((2,)), dma((2, 4)), dma((1,)), dma((8,)),
            dma((2, 2)), dma((2, 2, 14)), dma((2,)), dma((2, 16)),
            dma((2, 2)), dma((2, 2, 14)), dma((2,)), dma((2, 4)),
            dma((1,)), dma((1,)), dma((10,)),
        ],
        compiler_params=pltpu.CompilerParams(collective_id=0, has_side_effects=True,
                                             vmem_limit_bytes=VMEM_LIMIT),
        name='moe',
    )(x0, dy, *meta, *ws)


def _tn(a, b):
    return lax.dot_general(a, b, (((0,), (0,)), ((), ())), preferred_element_type=F32)


def _wgrad_kernel(x2_r, dx0_r, dgr, ia_ref, ib_ref, gc, xg_h, zg_h, h_h, d_h,
                  x2_o, dx0_o, o1a, o3a, o2a, o1b, o3b, o2b, dga, dgb,
                  x, z, h, d, o1, o3, o2, isem, osem):
    T = x2_r.shape[0]
    F = h.shape[3]
    def icopy(l, i, e=0):
        if i == 1:
            return pltpu.make_async_copy(d_h.at[l, e], d.at[l, e], isem.at[l, 1 + e])
        src, dst, k = ((xg_h, x, 0), None, (zg_h, z, 3), (h_h, h, 4))[i]
        return pltpu.make_async_copy(src.at[l], dst.at[l], isem.at[l, k])
    for l in (1, 0):
        icopy(l, 0).start()
        icopy(l, 1, 0).start()
        icopy(l, 1, 1).start()
        icopy(l, 2).start()
        icopy(l, 3).start()
    x2_o[...] = x2_r[...]
    dx0_o[...] = dx0_r[...]
    for l, ir, o in ((0, ia_ref, dga), (1, ib_ref, dgb)):
        idx = ir[...]
        acc = jnp.zeros((8, T), F32)
        for i in range(16):
            for e in range(2):
                row = dgr[8 * i + 2 * l + e:8 * i + 2 * l + e + 1, 0:T]
                acc = jnp.where(idx == 2 * i + e, row, acc)
        o[...] = acc
    outrefs = ((o1a, o3a, o2a), (o1b, o3b, o2b))

    def ocopy(l, i, e):
        return pltpu.make_async_copy((o1, o3, o2)[i].at[l, e], outrefs[l][i].at[e], osem.at[l, e, i])
    for l in (1, 0):
        icopy(l, 0).wait()

        @pl.loop(0, 2)
        def _(e):
            icopy(l, 1, e).wait()
            v = _tn(x[l], d[l, e])
            o1[l, e] = v[:, :F]
            o3[l, e] = v[:, F:]
            ocopy(l, 0, e).start()
            ocopy(l, 1, e).start()
        icopy(l, 2).wait()
        icopy(l, 3).wait()

        @pl.loop(0, 2)
        def _(e):
            g = jnp.where(e == 0, gc[:, 2 * l:2 * l + 1], gc[:, 2 * l + 1:2 * l + 2])
            do = jnp.where(g >= 0, g * z[l].astype(F32), 0.0).astype(BF)
            o2[l, e] = _tn(h[l, e], do)
            ocopy(l, 2, e).start()
    for l in range(2):
        for e in range(2):
            for i in range(3):
                ocopy(l, i, e).wait()


def _wgrad(x2, dx0, dgr, meta, gc, xg, zg, h, d):
    T = x2.shape[0]
    _, N, D = xg.shape
    EL, F = h.shape[1], h.shape[3]
    S = jax.ShapeDtypeStruct
    vm = pl.BlockSpec(memory_space=pltpu.VMEM)
    hb = pl.BlockSpec(memory_space=pl.ANY)
    dma = pltpu.SemaphoreType.DMA
    up, dn = S((EL, D, F), F32), S((EL, F, D), F32)
    return pl.pallas_call(
        _wgrad_kernel,
        out_shape=(S((T, D), BF), S((T, D), BF), up, up, dn, up, up, dn, S((8, T), F32), S((8, T), F32)),
        in_specs=[vm] * 6 + [hb] * 4,
        out_specs=(vm, vm) + (hb,) * 6 + (vm, vm),
        scratch_shapes=[
            pltpu.VMEM((2, N, D), BF), pltpu.VMEM((2, N, D), BF), pltpu.VMEM((2, EL, N, F), BF),
            pltpu.VMEM((2, EL, N, 2 * F), BF),
            pltpu.VMEM((2, EL, D, F), F32), pltpu.VMEM((2, EL, D, F), F32), pltpu.VMEM((2, EL, F, D), F32),
            dma((2, 5)), dma((2, EL, 3)),
        ],
        compiler_params=pltpu.CompilerParams(vmem_limit_bytes=VMEM_LIMIT),
        name='wgrad',
    )(x2, dx0, dgr, *meta, gc, xg, zg, h, d)


def solution(mesh):
    tok = P(('dp', 'ep'))
    wsp = P('ep')

    def body(x0, idx_a, g_a, idx_b, g_b, dy, *ws):
        T, D = x0.shape
        N = 16 * T
        ids = (idx_a.T, idx_b.T)
        x2, dx0, dgr, gc, xg, zg, h, d = _main(x0, dy, ids + (g_a.T, g_b.T), ws)
        r = _wgrad(x2, dx0, dgr, ids, gc, xg.reshape(2, N, D), zg.reshape(2, N, D), h, d)
        return tuple(r[:8]) + (r[8].T, r[9].T)

    return jax.shard_map(body, mesh=mesh,
                         in_specs=(tok,) * 6 + (wsp,) * 6,
                         out_specs=(tok,) * 10,
                         check_vma=False)
```

```python
import jax
import jax.numpy as jnp
from jax import lax
from jax.experimental import pallas as pl
from jax.experimental.pallas import tpu as pltpu
from jax.sharding import PartitionSpec as P

F32 = jnp.float32
BF = jnp.bfloat16
MESH = pl.DeviceIdType.MESH
VMEM_LIMIT = 67043328

REL = (-1, 1, -2, 2, -3, 3, 4, 0)
OWN = 7
UP = (6, 5, 3, 1, 7)
DOWN = (6, 4, 2, 0, 7)


def _ring_pos(ep):
    z, y = ep // 4, (ep // 2) % 2
    return z + y * (7 - 2 * z)


def _ring_ep(pos, core):
    y = pos // 4
    z = pos + y * (7 - 2 * pos)
    return z * 4 + y * 2 + core


def _nt(a, b):
    return lax.dot_general(a, b, (((1,), (1,)), ((), ())), preferred_element_type=F32)


def _nn(a, b):
    return jnp.dot(a, b, preferred_element_type=F32)


def _main_kernel(x0_ref, dy_ref, ia_ref, ib_ref, ga_ref, gb_ref, w1a_h, w3a_h, w2a_h, w1b_h, w3b_h, w2b_h,
                 x2_ref, dx0_ref, dgr_ref, gc_ref, xg_o, zg_o, h_o, d13_o,
                 w13, w2, xg, ps, dr, ru, rd, a13s, hs, d13s, gq, gtr, dgc, dgs, tmp,
                 wsem, gq_s, gq_r, gx_s, gx_r, ag_s, ag_r, ax_s, ax_r, rs_s, rs_r, rx_s, rx_r, d_s, d_r, osem):
    T = x0_ref.shape[0]
    H = T // 2
    F = w2.shape[2]
    R = 4 * T
    xin = [pltpu.make_async_copy(r, xg.at[n, OWN, 0], osem.at[n])
           for n, r in enumerate((x0_ref, dy_ref))]
    for c in xin:
        c.start()
    me = lax.axis_index('ep')
    core = me % 2
    pos = _ring_pos(me)
    up = _ring_ep((pos + 1) % 8, core)
    down = _ring_ep((pos + 7) % 8, core)
    mate = me + 1 - 2 * core

    wcopies = []
    for l, refs in enumerate(((w1a_h, w3a_h, w2a_h), (w1b_h, w3b_h, w2b_h))):
        for i, src in enumerate(refs):
            dst = w2.at[l] if i == 2 else w13.at[l, :, :, pl.ds(i * F, F)]
            c = pltpu.make_async_copy(src, dst, wsem.at[l * 3 + i])
            c.start()
            wcopies.append(c)

    bar = pltpu.get_barrier_semaphore()
    for dev in (up, down, mate):
        pl.semaphore_signal(bar, inc=1, device_id={'ep': dev}, device_id_type=MESH)
    for l, (ir, gr) in enumerate(((ia_ref, ga_ref), (ib_ref, gb_ref))):
        gq[OWN, 0, 8 * l:8 * l + 8, 0:T] = ir[...].astype(F32)
        gq[OWN, 0, 8 * l:8 * l + 8, T:2 * T] = gr[...]
    gtr[...] = jnp.full_like(gtr, -1.0)
    dgc[...] = jnp.zeros_like(dgc)
    for c in xin:
        c.wait()
    pl.semaphore_wait(bar, 3)

    def rcopy(src, dst, ss, rs, dev):
        return pltpu.make_async_remote_copy(src_ref=src, dst_ref=dst, send_sem=ss, recv_sem=rs,
                                            device_id={'ep': dev}, device_id_type=MESH)

    Q = H // 2

    def half(i):
        return pl.ds(i * H, H)

    def quarter(i, q):
        return pl.ds(i * H + q * Q, Q)

    AGSET = (0, 1, 0, 0)

    AU, AD = (7, 0, 2, 4, 6), (7, 1, 3, 5, 6)

    def ag_u(n, j, q):
        i, h, m = j // 2, quarter(j % 2, q), 2 * j + q
        return rcopy(xg.at[n, AU[i], 0, h], xg.at[n, AU[i + 1], 0, h], ag_s.at[AGSET[n], 0], ag_r.at[AGSET[n], 0, m], up)

    def ag_d(n, j, q):
        i, h, m = j // 2, quarter(1 - j % 2, q), 2 * j + q
        return rcopy(xg.at[n, AD[i], 0, h], xg.at[n, AD[i + 1], 0, h], ag_s.at[AGSET[n], 1], ag_r.at[AGSET[n], 1, m], down)

    def ag_m(n, k, hf):
        return rcopy(xg.at[n, k, 0, half(hf)], xg.at[n, k, 1, half(hf)],
                     ax_s.at[AGSET[n]], ax_r.at[AGSET[n], k * 2 + hf], mate)

    def gq_u(h):
        return rcopy(gq.at[AU[h], 0], gq.at[AU[h + 1], 0], gq_s.at[0], gq_r.at[0, h], up)

    def gq_d(h):
        return rcopy(gq.at[AD[h], 0], gq.at[AD[h + 1], 0], gq_s.at[1], gq_r.at[1, h], down)

    def gq_m(k):
        return rcopy(gq.at[k, 0], gq.at[k, 1], gx_s.at[0], gx_r.at[k], mate)

    def gq_step(h):
        def f():
            gq_u(h).wait_recv()
            if h < 3:
                gq_u(h + 1).start()
            gq_m(AU[h + 1]).start()
            if h < 3:
                gq_d(h).wait_recv()
                if h < 2:
                    gq_d(h + 1).start()
                gq_m(AD[h + 1]).start()
        return f

    def gates(ch):
        def f():
            for k in (2 * ch, 2 * ch + 1):
                gq_m(k).wait_recv()
                for plane in range(2):
                    for l in range(2):
                        t = gq[k, plane, 8 * l:8 * l + 8]
                        gt = pltpu.roll(t, T, 1)
                        for e in range(2):
                            row = 8 * (2 * k + plane) + 2 * l + e
                            mine = (2 * me + e).astype(F32)
                            gtr[row:row + 1] = jnp.max(jnp.where(t == mine, gt, -1.0), axis=0, keepdims=True)
            gct = gtr[...].T
            for b in range(4 * ch, 4 * ch + 4):
                gc_ref[b * T:(b + 1) * T, 0:8] = gct[0:T, b * 8:b * 8 + 8]
        return f

    def ag_start(n):
        for j in range(2):
            for q in range(2):
                ag_u(n, j, q).start()
                ag_d(n, j, q).start()
        for hf in range(2):
            ag_m(n, OWN, hf).start()

    def ag_step(n, *js):
        def f():
            for j in js:
                for q in range(2):
                    ag_u(n, j, q).wait_recv()
                    if j + 2 < 7:
                        ag_u(n, j + 2, q).start()
                    ag_d(n, j, q).wait_recv()
                    if j + 2 < 7:
                        ag_d(n, j + 2, q).start()
                ag_m(n, AU[j // 2 + 1], j % 2).start()
                ag_m(n, AD[j // 2 + 1], 1 - j % 2).start()
        return f

    def ag_have(n, *ks):
        def f():
            for k in ks:
                for hf in range(2):
                    ag_m(n, k, hf).wait_recv()
        return f

    def sent(ref, sem):
        pltpu.make_async_copy(ref, ref, sem).wait()

    def ag_sent(n):
        for d in range(2):
            sent(xg.at[n, pl.ds(0, 7), 0, half(0)], ag_s.at[AGSET[n], d])
        sent(xg.at[n, :, 0], ax_s.at[AGSET[n]])

    def rs_l(n, b, ch):
        return rcopy(ps.at[b, pl.ds(2 * ch, 2), 1], dr.at[b, pl.ds(2 * ch, 2)],
                     rx_s.at[b], rx_r.at[b, ch], mate)

    def rs_u(n, b, j, q):
        m = 2 * j + q
        return rcopy(ps.at[b, UP[(j + 1) // 2], 0, quarter(j % 2, q)], ru.at[b, j, quarter(0, q)],
                     rs_s.at[b, 0], rs_r.at[b, 0, m], up)

    def rs_d(n, b, j, q):
        m = 2 * j + q
        return rcopy(ps.at[b, DOWN[(j + 1) // 2], 0, quarter(1 - j % 2, q)], rd.at[b, j, quarter(0, q)],
                     rs_s.at[b, 1], rs_r.at[b, 1, m], down)

    def rs_local(n, b, *chs):
        def f():
            for ch in chs:
                rs_l(n, b, ch).start()
        return f

    def rs_merge(n, b, *chs):
        def f():
            for ch in chs:
                rs_l(n, b, ch).wait_recv()
                for k in (2 * ch, 2 * ch + 1):
                    ps[b, k, 0] += dr[b, k]
        return f

    def rs_first(n, b):
        def f():
            for q in range(2):
                rs_u(n, b, 1, q).start()
                rs_d(n, b, 1, q).start()
        return f

    def rs_second(n, b):
        def f():
            for q in range(2):
                rs_u(n, b, 0, q).start()
                rs_d(n, b, 0, q).start()
        return f

    def rs_step(n, b, *js):
        def f():
            for j in js:
                k = (j + 3) // 2
                for q in range(2):
                    rs_u(n, b, j, q).wait_recv()
                    ps[b, UP[k], 0, quarter(j % 2, q)] += ru[b, j, quarter(0, q)]
                    if j + 2 < 7:
                        rs_u(n, b, j + 2, q).start()
                    rs_d(n, b, j, q).wait_recv()
                    ps[b, DOWN[k], 0, quarter(1 - j % 2, q)] += rd[b, j, quarter(0, q)]
                    if j + 2 < 7:
                        rs_d(n, b, j + 2, q).start()
        return f

    def rs_sent(n, b):
        for d in range(2):
            sent(ps.at[b, pl.ds(0, 7), 0, half(0)], rs_s.at[b, d])
        sent(ps.at[b, :, 1], rx_s.at[b])

    def token_loop(hooks, *stages):
        ns = len(stages)

        @pl.loop(0, 8 * ns)
        def _(it):
            for i, fs in hooks.items():
                @pl.when(it == i)
                def _():
                    for f in fs:
                        f()
            ch = it // (2 * ns)
            e = it % 2
            rows = pl.ds(pl.multiple_of(ch * R, R), R)
            if ns == 1:
                stages[0](ch, e, rows)
            else:
                for k in range(ns):
                    @pl.when((it // 2) % ns == k)
                    def _():
                        stages[k](ch, e, rows)

    def gate(l, e, rows):
        return jnp.where(e == 0, gc_ref[rows, 2 * l:2 * l + 1], gc_ref[rows, 2 * l + 1:2 * l + 2])

    def rows_of(n, ch):
        return xg[n, pl.ds(2 * ch, 2)].reshape(R, -1)

    def put(b, ch, e, v):
        s = pl.ds(2 * ch, 2)
        ps[b, s] = jnp.where(e == 0, 0.0, ps[b, s]) + v.reshape(2, 2, T, v.shape[-1])

    def act(a1):
        sg = 1.0 / (1.0 + jnp.exp(-a1))
        return sg, a1 * sg

    def forward(l, n, b, ch, e, rows, a13s):
        g = gate(l, e, rows)
        a13 = _nn(rows_of(n, ch), w13[l, e])
        a13s[...] = a13
        sg, sl = act(a13[:, :F])
        h = jnp.where(g >= 0, sl * a13[:, F:], 0.0).astype(BF)
        hs[l, e, rows] = h
        put(b, ch, e, g * _nn(h, w2[l, e]).astype(BF).astype(F32))

    def backward(l, nz, b, ch, e, rows, a13s):
        g = gate(l, e, rows)
        a1 = a13s[:, :F]
        a3 = a13s[:, F:]
        sg, sl = act(a1)
        h = hs[l, e, rows]
        r = _nt(rows_of(nz, ch), w2[l, e])
        dg = jnp.sum(h.astype(F32) * r, axis=1, keepdims=True)
        lane = lax.broadcasted_iota(jnp.int32, (R, 8), 1)
        dgc[rows, 0:8] = jnp.where(lane == 2 * l + e, dg, dgc[rows, 0:8])
        dh = g * r
        da3 = jnp.where(g >= 0, dh * sl, 0.0).astype(BF)
        da1 = jnp.where(g >= 0, dh * a3 * sg * (1.0 + a1 * (1.0 - sg)), 0.0).astype(BF)
        d13s[l, e, rows, 0:F] = da1
        d13s[l, e, rows, F:2 * F] = da3
        put(b, ch, e, _nt(d13s[l, e, rows], w13[l, e]).astype(BF).astype(F32))

    gq_u(0).start()
    gq_d(0).start()
    gq_m(OWN).start()
    ag_start(0)
    for c in wcopies[:3]:
        c.wait()
    token_loop({
        0: [gq_step(0), ag_step(0, 0, 1), gates(0), ag_have(0, 0, 1)],
        1: [gq_step(1), ag_step(0, 2)],
        2: [ag_step(0, 3), gates(1), ag_have(0, 2, 3), rs_local(0, 0, 0)],
        3: [gq_step(2), ag_step(0, 4), lambda: ag_start(1)],
        4: [ag_step(0, 5), gates(2), ag_have(0, 4, 5)],
        5: [gq_step(3), ag_step(0, 6), rs_local(0, 0, 1)],
        6: [rs_local(0, 0, 2), gates(3), ag_have(0, 6, 7)],
        7: [rs_merge(0, 0, 2), rs_first(0, 0), ag_step(1, 0, 1)],
    }, lambda ch, e, rows: forward(0, 0, 0, ch, e, rows, a13s.at[e, rows]))
    rs_local(0, 0, 3)()
    rs_merge(0, 0, 0, 1, 3)()
    rs_second(0, 0)()
    rs_step(0, 0, 1, 0, 3, 2, 5, 4)()
    ag_step(1, 2, 3)()
    rs_step(0, 0, 6)()
    xg[2, OWN, 0] = (xg[0, OWN, 0].astype(F32) + ps[0, OWN, 0]).astype(BF)
    ag_sent(0)
    ag_start(2)
    rs_sent(0, 0)
    for c in wcopies[3:]:
        c.wait()

    token_loop({
        0: [ag_step(2, 0, 1), ag_have(2, 0, 1)],
        1: [ag_step(2, 2), ag_step(1, 4)],
        2: [ag_step(2, 3), ag_step(1, 5), ag_have(1, 0, 1)],
        3: [ag_step(2, 4), ag_step(1, 6)],
        4: [ag_step(2, 5), ag_have(2, 2, 3), rs_local(2, 0, 0), rs_local(1, 1, 0)],
        5: [ag_step(2, 6)],
        6: [ag_have(1, 2, 3)],
        8: [ag_have(2, 4, 5), rs_local(2, 0, 1), rs_local(1, 1, 1)],
        10: [rs_local(1, 1, 2), ag_have(1, 4, 5), rs_merge(1, 1, 0, 1)],
        11: [rs_merge(1, 1, 2), rs_first(1, 1)],
        12: [rs_local(2, 0, 2), ag_have(2, 6, 7)],
        13: [rs_merge(2, 0, 2), rs_first(2, 0), rs_merge(2, 0, 0, 1)],
        14: [rs_local(1, 1, 3), ag_have(1, 6, 7)],
        15: [rs_merge(1, 1, 3), rs_second(1, 1)],
    }, lambda ch, e, rows: forward(1, 2, 1, ch, e, rows, tmp.at[e]),
        lambda ch, e, rows: backward(1, 1, 0, ch, e, rows, tmp.at[e]))
    rs_local(2, 0, 3)()
    outs = []

    def out(src, dst, i):
        c = pltpu.make_async_copy(src, dst, osem.at[i])
        c.start()
        outs.append(c)
    for i, (sr, ds) in enumerate(((hs, h_o), (d13s, d13_o))):
        out(sr.at[1], ds.at[1], i)
    out(xg.at[0], xg_o.at[0], 3)
    out(xg.at[2], xg_o.at[1], 4)
    out(xg.at[1], zg_o.at[1], 5)
    rs_merge(2, 0, 3)()
    rs_second(2, 0)()
    rs_step(2, 0, 1, 0, 3, 2, 5, 4)()
    rs_step(2, 0, 6)()
    xg[3, OWN, 0] = (xg[1, OWN, 0].astype(F32) + ps[0, OWN, 0]).astype(BF)
    ag_sent(2)
    ag_start(3)
    rs_step(1, 1, 1)()
    rs_sent(2, 0)

    token_loop({
        0: [ag_step(3, 0, 1), ag_have(3, 0, 1)],
        1: [ag_step(3, 2)],
        2: [ag_step(3, 3), ag_have(3, 2, 3), rs_local(3, 0, 0)],
        3: [ag_step(3, 4)],
        4: [ag_step(3, 5), rs_step(1, 1, 0), ag_have(3, 4, 5)],
        5: [ag_step(3, 6), rs_step(1, 1, 3), rs_local(3, 0, 1)],
        6: [rs_local(3, 0, 2), ag_have(3, 6, 7)],
        7: [rs_merge(3, 0, 2), rs_first(3, 0)],
    }, lambda ch, e, rows: backward(0, 3, 0, ch, e, rows, a13s.at[e, rows]))
    rs_local(3, 0, 3)()
    out(xg.at[3], zg_o.at[0], 6)
    for i, (sr, ds) in enumerate(((hs, h_o), (d13s, d13_o))):
        out(sr.at[0], ds.at[0], 7 + i)
    rs_merge(3, 0, 0, 1, 3)()
    rs_second(3, 0)()

    for k in range(8):
        t = dgc[k * 2 * T:(k + 1) * 2 * T].T[0:8]
        dgs[k * 16:k * 16 + 8] = t
        dgs[k * 16 + 8:k * 16 + 16] = pltpu.roll(t, T, 1)
        q = (pos + REL[k] + 8) % 8
        for plane in range(2):
            b = k * 2 + plane
            if k == OWN and plane == 0:
                continue
            dev = _ring_ep(q, core + plane * (1 - 2 * core))
            c = rcopy(dgs.at[pl.ds(b * 8, 8)], dgr_ref.at[pl.ds(me * 8, 8)], d_s.at[0], d_r.at[0], dev)
            c.start()
    dgr_ref[pl.ds(pl.multiple_of(me * 8, 8), 8)] = dgs[16 * OWN:16 * OWN + 8]

    rs_step(3, 0, 1, 0)()
    rs_step(1, 1, 2)()
    rs_step(3, 0, 3, 2)()
    rs_step(1, 1, 5, 4)()
    rs_step(3, 0, 5, 4)()
    rs_step(1, 1, 6)()
    rs_step(3, 0, 6)()
    dx0_ref[...] = (xg[3, OWN, 0].astype(F32) + ps[0, OWN, 0]).astype(BF)
    x2_ref[...] = (xg[2, OWN, 0].astype(F32) + ps[1, OWN, 0]).astype(BF)
    sent(dgs.at[pl.ds(0, 120)], d_r.at[0])
    sent(dgs.at[pl.ds(0, 120)], d_s.at[0])
    sent(gq.at[pl.ds(0, 4), 0], gq_s.at[0])
    sent(gq.at[pl.ds(0, 3), 0], gq_s.at[1])
    sent(gq.at[:, 0], gx_s.at[0])
    for n in (1, 3):
        ag_sent(n)
    rs_sent(1, 1)
    rs_sent(3, 0)
    for c in outs:
        c.wait()


def _main(x0, dy, meta, ws):
    T, D = x0.shape
    EL, _, F = ws[0].shape
    N = 16 * T
    S = jax.ShapeDtypeStruct
    vm = pl.BlockSpec(memory_space=pltpu.VMEM)
    hb = pl.BlockSpec(memory_space=pl.ANY)
    dma = pltpu.SemaphoreType.DMA
    return pl.pallas_call(
        _main_kernel,
        out_shape=(S((T, D), BF), S((T, D), BF), S((128, 128), F32), S((N, 128), F32),
                   S((2, 8, 2, T, D), BF), S((2, 8, 2, T, D), BF),
                   S((2, EL, N, F), BF), S((2, EL, N, 2 * F), BF)),
        in_specs=[hb] * 2 + [vm] * 4 + [hb] * 6,
        out_specs=(vm, vm, vm, vm) + (hb,) * 4,
        scratch_shapes=[
            pltpu.VMEM((2, EL, D, 2 * F), BF), pltpu.VMEM((2, EL, F, D), BF),
            pltpu.VMEM((4, 8, 2, T, D), BF),
            pltpu.VMEM((2, 8, 2, T, D), F32), pltpu.VMEM((2, 8, T, D), F32),
            pltpu.VMEM((2, 7, T // 2, D), F32), pltpu.VMEM((2, 7, T // 2, D), F32),
            pltpu.VMEM((EL, N, 2 * F), F32),
            pltpu.VMEM((2, EL, N, F), BF), pltpu.VMEM((2, EL, N, 2 * F), BF),
            pltpu.VMEM((8, 2, 16, 128), F32), pltpu.VMEM((128, 128), F32), pltpu.VMEM((N, 128), F32),
            pltpu.VMEM((128, 128), F32),
            pltpu.VMEM((EL, 4 * T, 2 * F), F32),
            dma((6,)), dma((2,)), dma((2, 4)), dma((1,)), dma((8,)),
            dma((2, 2)), dma((2, 2, 14)), dma((2,)), dma((2, 16)),
            dma((2, 2)), dma((2, 2, 14)), dma((2,)), dma((2, 4)),
            dma((1,)), dma((1,)), dma((10,)),
        ],
        compiler_params=pltpu.CompilerParams(collective_id=0, has_side_effects=True,
                                             vmem_limit_bytes=VMEM_LIMIT),
        name='moe',
    )(x0, dy, *meta, *ws)


def _tn(a, b):
    return lax.dot_general(a, b, (((0,), (0,)), ((), ())), preferred_element_type=F32)


def _wgrad_kernel(x2_r, dx0_r, dgr, ia_ref, ib_ref, gc, xg_h, zg_h, h_h, d_h,
                  x2_o, dx0_o, o1a, o3a, o2a, o1b, o3b, o2b, dga, dgb,
                  x, z, h, d, o1, o3, o2, isem, osem):
    T = x2_r.shape[0]
    F = h.shape[3]
    def icopy(l, i, e=0):
        if i == 1:
            return pltpu.make_async_copy(d_h.at[l, e], d.at[l, e], isem.at[l, 1 + e])
        src, dst, k = ((xg_h, x, 0), None, (zg_h, z, 3), (h_h, h, 4))[i]
        return pltpu.make_async_copy(src.at[l], dst.at[l], isem.at[l, k])
    for l in (1, 0):
        icopy(l, 0).start()
        icopy(l, 1, 0).start()
        icopy(l, 1, 1).start()
        icopy(l, 2).start()
        icopy(l, 3).start()
    x2_o[...] = x2_r[...]
    dx0_o[...] = dx0_r[...]
    for l, ir, o in ((0, ia_ref, dga), (1, ib_ref, dgb)):
        idx = ir[...]
        acc = jnp.zeros((8, T), F32)
        for i in range(16):
            for e in range(2):
                row = dgr[8 * i + 2 * l + e:8 * i + 2 * l + e + 1, 0:T]
                acc = jnp.where(idx == 2 * i + e, row, acc)
        o[...] = acc
    outrefs = ((o1a, o3a, o2a), (o1b, o3b, o2b))

    def ocopy(l, i, e):
        return pltpu.make_async_copy((o1, o3, o2)[i].at[l, e], outrefs[l][i].at[e], osem.at[l, e, i])
    for l in (1, 0):
        icopy(l, 0).wait()

        for e in range(2):
            icopy(l, 1, e).wait()
            v = _tn(x[l], d[l, e])
            o1[l, e] = v[:, :F]
            o3[l, e] = v[:, F:]
            ocopy(l, 0, e).start()
            ocopy(l, 1, e).start()
        icopy(l, 2).wait()
        icopy(l, 3).wait()

        for e in range(2):
            g = jnp.where(e == 0, gc[:, 2 * l:2 * l + 1], gc[:, 2 * l + 1:2 * l + 2])
            do = jnp.where(g >= 0, g * z[l].astype(F32), 0.0).astype(BF)
            o2[l, e] = _tn(h[l, e], do)
            ocopy(l, 2, e).start()
    for l in range(2):
        for e in range(2):
            for i in range(3):
                ocopy(l, i, e).wait()


def _wgrad(x2, dx0, dgr, meta, gc, xg, zg, h, d):
    T = x2.shape[0]
    _, N, D = xg.shape
    EL, F = h.shape[1], h.shape[3]
    S = jax.ShapeDtypeStruct
    vm = pl.BlockSpec(memory_space=pltpu.VMEM)
    hb = pl.BlockSpec(memory_space=pl.ANY)
    dma = pltpu.SemaphoreType.DMA
    up, dn = S((EL, D, F), F32), S((EL, F, D), F32)
    return pl.pallas_call(
        _wgrad_kernel,
        out_shape=(S((T, D), BF), S((T, D), BF), up, up, dn, up, up, dn, S((8, T), F32), S((8, T), F32)),
        in_specs=[vm] * 6 + [hb] * 4,
        out_specs=(vm, vm) + (hb,) * 6 + (vm, vm),
        scratch_shapes=[
            pltpu.VMEM((2, N, D), BF), pltpu.VMEM((2, N, D), BF), pltpu.VMEM((2, EL, N, F), BF),
            pltpu.VMEM((2, EL, N, 2 * F), BF),
            pltpu.VMEM((2, EL, D, F), F32), pltpu.VMEM((2, EL, D, F), F32), pltpu.VMEM((2, EL, F, D), F32),
            dma((2, 5)), dma((2, EL, 3)),
        ],
        compiler_params=pltpu.CompilerParams(vmem_limit_bytes=VMEM_LIMIT),
        name='wgrad',
    )(x2, dx0, dgr, *meta, gc, xg, zg, h, d)


def solution(mesh):
    tok = P(('dp', 'ep'))
    wsp = P('ep')

    def body(x0, idx_a, g_a, idx_b, g_b, dy, *ws):
        T, D = x0.shape
        N = 16 * T
        ids = (idx_a.T, idx_b.T)
        x2, dx0, dgr, gc, xg, zg, h, d = _main(x0, dy, ids + (g_a.T, g_b.T), ws)
        r = _wgrad(x2, dx0, dgr, ids, gc, xg.reshape(2, N, D), zg.reshape(2, N, D), h, d)
        return tuple(r[:8]) + (r[8].T, r[9].T)

    return jax.shard_map(body, mesh=mesh,
                         in_specs=(tok,) * 6 + (wsp,) * 6,
                         out_specs=(tok,) * 10,
                         check_vma=False)
```

```python
import jax
import jax.numpy as jnp
from jax import lax
from jax.experimental import pallas as pl
from jax.experimental.pallas import tpu as pltpu
from jax.sharding import PartitionSpec as P

F32 = jnp.float32
BF = jnp.bfloat16
MESH = pl.DeviceIdType.MESH
VMEM_LIMIT = 67043328

REL = (-1, 1, -2, 2, -3, 3, 4, 0)
OWN = 7
UP = (6, 5, 3, 1, 7)
DOWN = (6, 4, 2, 0, 7)


def _ring_pos(ep):
    z, y = ep // 4, (ep // 2) % 2
    return z + y * (7 - 2 * z)


def _ring_ep(pos, core):
    y = pos // 4
    z = pos + y * (7 - 2 * pos)
    return z * 4 + y * 2 + core


def _nt(a, b):
    return lax.dot_general(a, b, (((1,), (1,)), ((), ())), preferred_element_type=F32)


def _nn(a, b):
    return jnp.dot(a, b, preferred_element_type=F32)


def _main_kernel(x0_ref, dy_ref, ia_ref, ib_ref, ga_ref, gb_ref, w1a_h, w3a_h, w2a_h, w1b_h, w3b_h, w2b_h,
                 x2_ref, dx0_ref, dgr_ref, gc_ref, xg_o, zg_o, h_o, d13_o,
                 w13, w2, xg, ps, dr, ru, rd, a13s, hs, d13s, gq, gtr, dgc, dgs, tmp,
                 wsem, gq_s, gq_r, gx_s, gx_r, ag_s, ag_r, ax_s, ax_r, rs_s, rs_r, rx_s, rx_r, d_s, d_r, osem):
    T = x0_ref.shape[0]
    H = T // 2
    F = w2.shape[2]
    R = 4 * T
    xin = [pltpu.make_async_copy(r, xg.at[n, OWN, 0], osem.at[n])
           for n, r in enumerate((x0_ref, dy_ref))]
    for c in xin:
        c.start()
    me = lax.axis_index('ep')
    core = me % 2
    pos = _ring_pos(me)
    up = _ring_ep((pos + 1) % 8, core)
    down = _ring_ep((pos + 7) % 8, core)
    mate = me + 1 - 2 * core

    wcopies = []
    for l, refs in enumerate(((w1a_h, w3a_h, w2a_h), (w1b_h, w3b_h, w2b_h))):
        for i, src in enumerate(refs):
            dst = w2.at[l] if i == 2 else w13.at[l, :, :, pl.ds(i * F, F)]
            c = pltpu.make_async_copy(src, dst, wsem.at[l * 3 + i])
            c.start()
            wcopies.append(c)

    bar = pltpu.get_barrier_semaphore()
    for dev in (up, down, mate):
        pl.semaphore_signal(bar, inc=1, device_id={'ep': dev}, device_id_type=MESH)
    for l, (ir, gr) in enumerate(((ia_ref, ga_ref), (ib_ref, gb_ref))):
        gq[OWN, 0, 8 * l:8 * l + 8, 0:T] = ir[...].astype(F32)
        gq[OWN, 0, 8 * l:8 * l + 8, T:2 * T] = gr[...]
    gtr[...] = jnp.full_like(gtr, -1.0)
    dgc[...] = jnp.zeros_like(dgc)
    for c in xin:
        c.wait()
    pl.semaphore_wait(bar, 3)

    def rcopy(src, dst, ss, rs, dev):
        return pltpu.make_async_remote_copy(src_ref=src, dst_ref=dst, send_sem=ss, recv_sem=rs,
                                            device_id={'ep': dev}, device_id_type=MESH)

    Q = H // 2

    def half(i):
        return pl.ds(i * H, H)

    def quarter(i, q):
        return pl.ds(i * H + q * Q, Q)

    AGSET = (0, 1, 0, 0)

    AU, AD = (7, 0, 2, 4, 6), (7, 1, 3, 5, 6)

    def ag_u(n, j, q):
        i, h, m = j // 2, quarter(j % 2, q), 2 * j + q
        return rcopy(xg.at[n, AU[i], 0, h], xg.at[n, AU[i + 1], 0, h], ag_s.at[AGSET[n], 0], ag_r.at[AGSET[n], 0, m], up)

    def ag_d(n, j, q):
        i, h, m = j // 2, quarter(1 - j % 2, q), 2 * j + q
        return rcopy(xg.at[n, AD[i], 0, h], xg.at[n, AD[i + 1], 0, h], ag_s.at[AGSET[n], 1], ag_r.at[AGSET[n], 1, m], down)

    def ag_m(n, k, hf):
        return rcopy(xg.at[n, k, 0, half(hf)], xg.at[n, k, 1, half(hf)],
                     ax_s.at[AGSET[n]], ax_r.at[AGSET[n], k * 2 + hf], mate)

    def gq_u(h):
        return rcopy(gq.at[AU[h], 0], gq.at[AU[h + 1], 0], gq_s.at[0], gq_r.at[0, h], up)

    def gq_d(h):
        return rcopy(gq.at[AD[h], 0], gq.at[AD[h + 1], 0], gq_s.at[1], gq_r.at[1, h], down)

    def gq_m(k):
        return rcopy(gq.at[k, 0], gq.at[k, 1], gx_s.at[0], gx_r.at[k], mate)

    def gq_step(h):
        def f():
            gq_u(h).wait_recv()
            if h < 3:
                gq_u(h + 1).start()
            gq_m(AU[h + 1]).start()
            if h < 3:
                gq_d(h).wait_recv()
                if h < 2:
                    gq_d(h + 1).start()
                gq_m(AD[h + 1]).start()
        return f

    def gates(ch):
        def f():
            for k in (2 * ch, 2 * ch + 1):
                gq_m(k).wait_recv()
                for plane in range(2):
                    for l in range(2):
                        t = gq[k, plane, 8 * l:8 * l + 8]
                        gt = pltpu.roll(t, T, 1)
                        for e in range(2):
                            row = 8 * (2 * k + plane) + 2 * l + e
                            mine = (2 * me + e).astype(F32)
                            gtr[row:row + 1] = jnp.max(jnp.where(t == mine, gt, -1.0), axis=0, keepdims=True)
            gct = gtr[...].T
            for b in range(4 * ch, 4 * ch + 4):
                gc_ref[b * T:(b + 1) * T, 0:8] = gct[0:T, b * 8:b * 8 + 8]
        return f

    def ag_start(n):
        for j in range(2):
            for q in range(2):
                ag_u(n, j, q).start()
                ag_d(n, j, q).start()
        for hf in range(2):
            ag_m(n, OWN, hf).start()

    def ag_step(n, *js):
        def f():
            for j in js:
                for q in range(2):
                    ag_u(n, j, q).wait_recv()
                    if j + 2 < 7:
                        ag_u(n, j + 2, q).start()
                    ag_d(n, j, q).wait_recv()
                    if j + 2 < 7:
                        ag_d(n, j + 2, q).start()
                ag_m(n, AU[j // 2 + 1], j % 2).start()
                ag_m(n, AD[j // 2 + 1], 1 - j % 2).start()
        return f

    def ag_have(n, *ks):
        def f():
            for k in ks:
                for hf in range(2):
                    ag_m(n, k, hf).wait_recv()
        return f

    def sent(ref, sem):
        pltpu.make_async_copy(ref, ref, sem).wait()

    def ag_sent(n):
        for d in range(2):
            sent(xg.at[n, pl.ds(0, 7), 0, half(0)], ag_s.at[AGSET[n], d])
        sent(xg.at[n, :, 0], ax_s.at[AGSET[n]])

    def rs_l(n, b, ch):
        return rcopy(ps.at[b, pl.ds(2 * ch, 2), 1], dr.at[b, pl.ds(2 * ch, 2)],
                     rx_s.at[b], rx_r.at[b, ch], mate)

    def rs_u(n, b, j, q):
        m = 2 * j + q
        return rcopy(ps.at[b, UP[(j + 1) // 2], 0, quarter(j % 2, q)], ru.at[b, j, quarter(0, q)],
                     rs_s.at[b, 0], rs_r.at[b, 0, m], up)

    def rs_d(n, b, j, q):
        m = 2 * j + q
        return rcopy(ps.at[b, DOWN[(j + 1) // 2], 0, quarter(1 - j % 2, q)], rd.at[b, j, quarter(0, q)],
                     rs_s.at[b, 1], rs_r.at[b, 1, m], down)

    def rs_local(n, b, *chs):
        def f():
            for ch in chs:
                rs_l(n, b, ch).start()
        return f

    def rs_merge(n, b, *chs):
        def f():
            for ch in chs:
                rs_l(n, b, ch).wait_recv()
                for k in (2 * ch, 2 * ch + 1):
                    ps[b, k, 0] += dr[b, k]
        return f

    def rs_first(n, b):
        def f():
            for q in range(2):
                rs_u(n, b, 1, q).start()
                rs_d(n, b, 1, q).start()
        return f

    def rs_second(n, b):
        def f():
            for q in range(2):
                rs_u(n, b, 0, q).start()
                rs_d(n, b, 0, q).start()
        return f

    def rs_step(n, b, *js):
        def f():
            for j in js:
                k = (j + 3) // 2
                for q in range(2):
                    rs_u(n, b, j, q).wait_recv()
                    ps[b, UP[k], 0, quarter(j % 2, q)] += ru[b, j, quarter(0, q)]
                    if j + 2 < 7:
                        rs_u(n, b, j + 2, q).start()
                    rs_d(n, b, j, q).wait_recv()
                    ps[b, DOWN[k], 0, quarter(1 - j % 2, q)] += rd[b, j, quarter(0, q)]
                    if j + 2 < 7:
                        rs_d(n, b, j + 2, q).start()
        return f

    def rs_sent(n, b):
        for d in range(2):
            sent(ps.at[b, pl.ds(0, 7), 0, half(0)], rs_s.at[b, d])
        sent(ps.at[b, :, 1], rx_s.at[b])

    def token_loop(hooks, *stages):
        ns = len(stages)

        @pl.loop(0, 8 * ns)
        def _(it):
            for i, fs in hooks.items():
                @pl.when(it == i)
                def _():
                    for f in fs:
                        f()
            ch = it // (2 * ns)
            e = it % 2
            rows = pl.ds(pl.multiple_of(ch * R, R), R)
            if ns == 1:
                stages[0](ch, e, rows)
            else:
                for k in range(ns):
                    @pl.when((it // 2) % ns == k)
                    def _():
                        stages[k](ch, e, rows)

    def pair_loop(hooks, *stages):
        ns = len(stages)

        @pl.loop(0, 4 * ns)
        def _(it):
            for i, fs in hooks.items():
                @pl.when(it == i)
                def _():
                    for f in fs:
                        f()
            ch = it // ns
            rows = pl.ds(pl.multiple_of(ch * R, R), R)
            for k in range(ns):
                @pl.when(it % ns == k)
                def _():
                    for e in range(2):
                        stages[k](ch, e, rows)

    def gate(l, e, rows):
        if isinstance(e, int):
            return gc_ref[rows, 2 * l + e:2 * l + e + 1]
        return jnp.where(e == 0, gc_ref[rows, 2 * l:2 * l + 1], gc_ref[rows, 2 * l + 1:2 * l + 2])

    def rows_of(n, ch):
        return xg[n, pl.ds(2 * ch, 2)].reshape(R, -1)

    def put(b, ch, e, v):
        s = pl.ds(2 * ch, 2)
        v = v.reshape(2, 2, T, v.shape[-1])
        if isinstance(e, int):
            ps[b, s] = v if e == 0 else ps[b, s] + v
        else:
            ps[b, s] = jnp.where(e == 0, 0.0, ps[b, s]) + v

    def act(a1):
        sg = 1.0 / (1.0 + jnp.exp(-a1))
        return sg, a1 * sg

    def forward(l, n, b, ch, e, rows, a13s):
        g = gate(l, e, rows)
        a13 = _nn(rows_of(n, ch), w13[l, e])
        a13s[...] = a13
        sg, sl = act(a13[:, :F])
        h = jnp.where(g >= 0, sl * a13[:, F:], 0.0).astype(BF)
        hs[l, e, rows] = h
        put(b, ch, e, g * _nn(h, w2[l, e]).astype(BF).astype(F32))

    def backward(l, nz, b, ch, e, rows, a13s):
        g = gate(l, e, rows)
        a1 = a13s[:, :F]
        a3 = a13s[:, F:]
        sg, sl = act(a1)
        h = hs[l, e, rows]
        r = _nt(rows_of(nz, ch), w2[l, e])
        dg = jnp.sum(h.astype(F32) * r, axis=1, keepdims=True)
        lane = lax.broadcasted_iota(jnp.int32, (R, 8), 1)
        dgc[rows, 0:8] = jnp.where(lane == 2 * l + e, dg, dgc[rows, 0:8])
        dh = g * r
        da3 = jnp.where(g >= 0, dh * sl, 0.0).astype(BF)
        da1 = jnp.where(g >= 0, dh * a3 * sg * (1.0 + a1 * (1.0 - sg)), 0.0).astype(BF)
        d13s[l, e, rows, 0:F] = da1
        d13s[l, e, rows, F:2 * F] = da3
        put(b, ch, e, _nt(d13s[l, e, rows], w13[l, e]).astype(BF).astype(F32))

    gq_u(0).start()
    gq_d(0).start()
    gq_m(OWN).start()
    ag_start(0)
    for c in wcopies[:3]:
        c.wait()
    token_loop({
        0: [gq_step(0), ag_step(0, 0, 1), gates(0), ag_have(0, 0, 1)],
        1: [gq_step(1), ag_step(0, 2)],
        2: [ag_step(0, 3), gates(1), ag_have(0, 2, 3), rs_local(0, 0, 0)],
        3: [gq_step(2), ag_step(0, 4), lambda: ag_start(1)],
        4: [ag_step(0, 5), gates(2), ag_have(0, 4, 5)],
        5: [gq_step(3), ag_step(0, 6), rs_local(0, 0, 1)],
        6: [rs_local(0, 0, 2), gates(3), ag_have(0, 6, 7)],
        7: [rs_merge(0, 0, 2), rs_first(0, 0), ag_step(1, 0, 1)],
    }, lambda ch, e, rows: forward(0, 0, 0, ch, e, rows, a13s.at[e, rows]))
    rs_local(0, 0, 3)()
    rs_merge(0, 0, 0, 1, 3)()
    rs_second(0, 0)()
    rs_step(0, 0, 1, 0, 3, 2, 5, 4)()
    ag_step(1, 2, 3)()
    rs_step(0, 0, 6)()
    xg[2, OWN, 0] = (xg[0, OWN, 0].astype(F32) + ps[0, OWN, 0]).astype(BF)
    ag_sent(0)
    ag_start(2)
    rs_sent(0, 0)
    for c in wcopies[3:]:
        c.wait()

    pair_loop({
        0: [ag_step(2, 0, 1), ag_have(2, 0, 1)],
        1: [ag_step(2, 2, 3), ag_step(1, 4, 5), ag_have(1, 0, 1)],
        2: [ag_step(2, 4), ag_step(1, 6), ag_have(2, 2, 3), rs_local(2, 0, 0), rs_local(1, 1, 0)],
        3: [ag_step(2, 5, 6), ag_have(1, 2, 3)],
        4: [ag_have(2, 4, 5), rs_local(2, 0, 1), rs_local(1, 1, 1)],
        5: [rs_local(1, 1, 2), ag_have(1, 4, 5), rs_merge(1, 1, 0, 1, 2), rs_first(1, 1)],
        6: [rs_local(2, 0, 2), ag_have(2, 6, 7), rs_merge(2, 0, 0, 1)],
        7: [rs_merge(2, 0, 2), rs_first(2, 0), rs_local(1, 1, 3), ag_have(1, 6, 7), rs_merge(1, 1, 3), rs_second(1, 1)],
    }, lambda ch, e, rows: forward(1, 2, 1, ch, e, rows, tmp.at[e]),
        lambda ch, e, rows: backward(1, 1, 0, ch, e, rows, tmp.at[e]))
    rs_local(2, 0, 3)()
    outs = []

    def out(src, dst, i):
        c = pltpu.make_async_copy(src, dst, osem.at[i])
        c.start()
        outs.append(c)
    for i, (sr, ds) in enumerate(((hs, h_o), (d13s, d13_o))):
        out(sr.at[1], ds.at[1], i)
    out(xg.at[0], xg_o.at[0], 3)
    out(xg.at[2], xg_o.at[1], 4)
    out(xg.at[1], zg_o.at[1], 5)
    rs_merge(2, 0, 3)()
    rs_second(2, 0)()
    rs_step(2, 0, 1, 0, 3, 2, 5, 4)()
    rs_step(2, 0, 6)()
    xg[3, OWN, 0] = (xg[1, OWN, 0].astype(F32) + ps[0, OWN, 0]).astype(BF)
    ag_sent(2)
    ag_start(3)
    rs_step(1, 1, 1)()
    rs_sent(2, 0)

    token_loop({
        0: [ag_step(3, 0, 1), ag_have(3, 0, 1)],
        1: [ag_step(3, 2)],
        2: [ag_step(3, 3), ag_have(3, 2, 3), rs_local(3, 0, 0)],
        3: [ag_step(3, 4)],
        4: [ag_step(3, 5), rs_step(1, 1, 0), ag_have(3, 4, 5)],
        5: [ag_step(3, 6), rs_step(1, 1, 3), rs_local(3, 0, 1)],
        6: [rs_local(3, 0, 2), ag_have(3, 6, 7)],
        7: [rs_merge(3, 0, 2), rs_first(3, 0)],
    }, lambda ch, e, rows: backward(0, 3, 0, ch, e, rows, a13s.at[e, rows]))
    rs_local(3, 0, 3)()
    out(xg.at[3], zg_o.at[0], 6)
    for i, (sr, ds) in enumerate(((hs, h_o), (d13s, d13_o))):
        out(sr.at[0], ds.at[0], 7 + i)
    rs_merge(3, 0, 0, 1, 3)()
    rs_second(3, 0)()

    for k in range(8):
        t = dgc[k * 2 * T:(k + 1) * 2 * T].T[0:8]
        dgs[k * 16:k * 16 + 8] = t
        dgs[k * 16 + 8:k * 16 + 16] = pltpu.roll(t, T, 1)
        q = (pos + REL[k] + 8) % 8
        for plane in range(2):
            b = k * 2 + plane
            if k == OWN and plane == 0:
                continue
            dev = _ring_ep(q, core + plane * (1 - 2 * core))
            c = rcopy(dgs.at[pl.ds(b * 8, 8)], dgr_ref.at[pl.ds(me * 8, 8)], d_s.at[0], d_r.at[0], dev)
            c.start()
    dgr_ref[pl.ds(pl.multiple_of(me * 8, 8), 8)] = dgs[16 * OWN:16 * OWN + 8]

    rs_step(3, 0, 1, 0)()
    rs_step(1, 1, 2)()
    rs_step(3, 0, 3, 2)()
    rs_step(1, 1, 5, 4)()
    rs_step(3, 0, 5, 4)()
    rs_step(1, 1, 6)()
    rs_step(3, 0, 6)()
    dx0_ref[...] = (xg[3, OWN, 0].astype(F32) + ps[0, OWN, 0]).astype(BF)
    x2_ref[...] = (xg[2, OWN, 0].astype(F32) + ps[1, OWN, 0]).astype(BF)
    sent(dgs.at[pl.ds(0, 120)], d_r.at[0])
    sent(dgs.at[pl.ds(0, 120)], d_s.at[0])
    sent(gq.at[pl.ds(0, 4), 0], gq_s.at[0])
    sent(gq.at[pl.ds(0, 3), 0], gq_s.at[1])
    sent(gq.at[:, 0], gx_s.at[0])
    for n in (1, 3):
        ag_sent(n)
    rs_sent(1, 1)
    rs_sent(3, 0)
    for c in outs:
        c.wait()


def _main(x0, dy, meta, ws):
    T, D = x0.shape
    EL, _, F = ws[0].shape
    N = 16 * T
    S = jax.ShapeDtypeStruct
    vm = pl.BlockSpec(memory_space=pltpu.VMEM)
    hb = pl.BlockSpec(memory_space=pl.ANY)
    dma = pltpu.SemaphoreType.DMA
    return pl.pallas_call(
        _main_kernel,
        out_shape=(S((T, D), BF), S((T, D), BF), S((128, 128), F32), S((N, 128), F32),
                   S((2, 8, 2, T, D), BF), S((2, 8, 2, T, D), BF),
                   S((2, EL, N, F), BF), S((2, EL, N, 2 * F), BF)),
        in_specs=[hb] * 2 + [vm] * 4 + [hb] * 6,
        out_specs=(vm, vm, vm, vm) + (hb,) * 4,
        scratch_shapes=[
            pltpu.VMEM((2, EL, D, 2 * F), BF), pltpu.VMEM((2, EL, F, D), BF),
            pltpu.VMEM((4, 8, 2, T, D), BF),
            pltpu.VMEM((2, 8, 2, T, D), F32), pltpu.VMEM((2, 8, T, D), F32),
            pltpu.VMEM((2, 7, T // 2, D), F32), pltpu.VMEM((2, 7, T // 2, D), F32),
            pltpu.VMEM((EL, N, 2 * F), F32),
            pltpu.VMEM((2, EL, N, F), BF), pltpu.VMEM((2, EL, N, 2 * F), BF),
            pltpu.VMEM((8, 2, 16, 128), F32), pltpu.VMEM((128, 128), F32), pltpu.VMEM((N, 128), F32),
            pltpu.VMEM((128, 128), F32),
            pltpu.VMEM((EL, 4 * T, 2 * F), F32),
            dma((6,)), dma((2,)), dma((2, 4)), dma((1,)), dma((8,)),
            dma((2, 2)), dma((2, 2, 14)), dma((2,)), dma((2, 16)),
            dma((2, 2)), dma((2, 2, 14)), dma((2,)), dma((2, 4)),
            dma((1,)), dma((1,)), dma((10,)),
        ],
        compiler_params=pltpu.CompilerParams(collective_id=0, has_side_effects=True,
                                             vmem_limit_bytes=VMEM_LIMIT),
        name='moe',
    )(x0, dy, *meta, *ws)


def _tn(a, b):
    return lax.dot_general(a, b, (((0,), (0,)), ((), ())), preferred_element_type=F32)


def _wgrad_kernel(x2_r, dx0_r, dgr, ia_ref, ib_ref, gc, xg_h, zg_h, h_h, d_h,
                  x2_o, dx0_o, o1a, o3a, o2a, o1b, o3b, o2b, dga, dgb,
                  x, z, h, d, o1, o3, o2, isem, osem):
    T = x2_r.shape[0]
    F = h.shape[3]
    def icopy(l, i, e=0):
        if i == 1:
            return pltpu.make_async_copy(d_h.at[l, e], d.at[l, e], isem.at[l, 1 + e])
        src, dst, k = ((xg_h, x, 0), None, (zg_h, z, 3), (h_h, h, 4))[i]
        return pltpu.make_async_copy(src.at[l], dst.at[l], isem.at[l, k])
    for l in (1, 0):
        icopy(l, 0).start()
        icopy(l, 1, 0).start()
        icopy(l, 1, 1).start()
        icopy(l, 2).start()
        icopy(l, 3).start()
    x2_o[...] = x2_r[...]
    dx0_o[...] = dx0_r[...]
    for l, ir, o in ((0, ia_ref, dga), (1, ib_ref, dgb)):
        idx = ir[...]
        acc = jnp.zeros((8, T), F32)
        for i in range(16):
            for e in range(2):
                row = dgr[8 * i + 2 * l + e:8 * i + 2 * l + e + 1, 0:T]
                acc = jnp.where(idx == 2 * i + e, row, acc)
        o[...] = acc
    outrefs = ((o1a, o3a, o2a), (o1b, o3b, o2b))

    def ocopy(l, i, e):
        return pltpu.make_async_copy((o1, o3, o2)[i].at[l, e], outrefs[l][i].at[e], osem.at[l, e, i])
    for l in (1, 0):
        icopy(l, 0).wait()

        for e in range(2):
            icopy(l, 1, e).wait()
            v = _tn(x[l], d[l, e])
            o1[l, e] = v[:, :F]
            o3[l, e] = v[:, F:]
            ocopy(l, 0, e).start()
            ocopy(l, 1, e).start()
        icopy(l, 2).wait()
        icopy(l, 3).wait()

        for e in range(2):
            g = jnp.where(e == 0, gc[:, 2 * l:2 * l + 1], gc[:, 2 * l + 1:2 * l + 2])
            do = jnp.where(g >= 0, g * z[l].astype(F32), 0.0).astype(BF)
            o2[l, e] = _tn(h[l, e], do)
            ocopy(l, 2, e).start()
    for l in range(2):
        for e in range(2):
            for i in range(3):
                ocopy(l, i, e).wait()


def _wgrad(x2, dx0, dgr, meta, gc, xg, zg, h, d):
    T = x2.shape[0]
    _, N, D = xg.shape
    EL, F = h.shape[1], h.shape[3]
    S = jax.ShapeDtypeStruct
    vm = pl.BlockSpec(memory_space=pltpu.VMEM)
    hb = pl.BlockSpec(memory_space=pl.ANY)
    dma = pltpu.SemaphoreType.DMA
    up, dn = S((EL, D, F), F32), S((EL, F, D), F32)
    return pl.pallas_call(
        _wgrad_kernel,
        out_shape=(S((T, D), BF), S((T, D), BF), up, up, dn, up, up, dn, S((8, T), F32), S((8, T), F32)),
        in_specs=[vm] * 6 + [hb] * 4,
        out_specs=(vm, vm) + (hb,) * 6 + (vm, vm),
        scratch_shapes=[
            pltpu.VMEM((2, N, D), BF), pltpu.VMEM((2, N, D), BF), pltpu.VMEM((2, EL, N, F), BF),
            pltpu.VMEM((2, EL, N, 2 * F), BF),
            pltpu.VMEM((2, EL, D, F), F32), pltpu.VMEM((2, EL, D, F), F32), pltpu.VMEM((2, EL, F, D), F32),
            dma((2, 5)), dma((2, EL, 3)),
        ],
        compiler_params=pltpu.CompilerParams(vmem_limit_bytes=VMEM_LIMIT),
        name='wgrad',
    )(x2, dx0, dgr, *meta, gc, xg, zg, h, d)


def solution(mesh):
    tok = P(('dp', 'ep'))
    wsp = P('ep')

    def body(x0, idx_a, g_a, idx_b, g_b, dy, *ws):
        T, D = x0.shape
        N = 16 * T
        ids = (idx_a.T, idx_b.T)
        x2, dx0, dgr, gc, xg, zg, h, d = _main(x0, dy, ids + (g_a.T, g_b.T), ws)
        r = _wgrad(x2, dx0, dgr, ids, gc, xg.reshape(2, N, D), zg.reshape(2, N, D), h, d)
        return tuple(r[:8]) + (r[8].T, r[9].T)

    return jax.shard_map(body, mesh=mesh,
                         in_specs=(tok,) * 6 + (wsp,) * 6,
                         out_specs=(tok,) * 10,
                         check_vma=False)
```
